32 devices in a mesh: blocks: 2 (over y), gz: 8 (over z, x), gy: 2 (over core).
Axes of the slice: x: 2, y: 2, z: 4, core: 2. Of those that a mesh axis runs over, the one named last changes fastest.
Arguments:
- view_a: float32 [256, 32, 512], P(('blocks', 'gz'), 'gy'), parts along dimension 0, may hold values from 0.5 to 2
- view_b_own: float32 [1024, 32, 128], P(('blocks', 'gz'), 'gy'), parts along dimension 0, may hold values from 0.5 to 2
- spread_a: float32 [3, 31], replicated, may hold values from 0.05 to 1
- spread_b: float32 [3, 31], replicated, may hold values from 0.05 to 1
Outputs:
- estimate: float32 [256, 32, 512], P(('blocks', 'gz'), 'gy'), parts along dimension 0
The draws below stay inside these ranges and needn't reach their ends.
There are 2 independent parts, one for each index of `blocks`. The reference program is written for one: setup_inputs(seed, part) draws one part's arguments, and reference() takes and returns one part's arrays. A program takes and returns all parts, laid end to end along the dimension named above; an argument that names none is the same for every part. Nothing has to cross between parts.
All inputs are finite; a program needn't handle non-finite values.
Results may differ from the reference program's by a relative error of at most 0.0001.
Values sent between devices are 32-bit elements; how exact they have to be, the bound alone decides.
A program may use at most 64 MiB of HBM per device.

```python
import math
import jax
import jax.numpy as jnp
from jax import lax

NX = 512
R = 15
ITERS = 1
NZ = 128
NY = 32


def level_of(key, extent, split, smallest, high):
    gain, own = 1.0, jax.random.fold_in(key, 6)
    for position, blocks in split:
        steps = jnp.exp(jax.random.uniform(jax.random.fold_in(own, position), (blocks,), jnp.float32, smallest / len(split), high / len(split)))
        gain = gain * jnp.repeat(steps, extent[position] // blocks).reshape([-1 if axis == position else 1 for axis in range(len(extent))])
    return gain


def setup_inputs(seed: int = 0, part: int = 0) -> dict:
    key_of = jax.random.split(jax.random.key(seed), 5)
    own_keys = jax.random.split(jax.random.fold_in(key_of[4], part), 5)
    return {
        "view_a": jnp.clip(0.5 + 1.5 * jax.random.uniform(own_keys[0], (NZ, NY, NX), jnp.float32) ** level_of(own_keys[0], (NZ, NY, NX), ((0, 8), (1, 2)), -0.2, 0.2), 0.5, 2.0),
        "view_b_own": jnp.clip(0.5 + 1.5 * jax.random.uniform(own_keys[1], (NX, NY, NZ), jnp.float32) ** level_of(own_keys[1], (NX, NY, NZ), ((0, 8), (1, 2)), -0.2, 0.2), 0.5, 2.0),
        "spread_a": jnp.clip(jnp.exp(jax.random.uniform(key_of[2], (3, 2 * R + 1), jnp.float32, math.log(0.05), math.log(1.0))), 0.05, 1.0),
        "spread_b": jnp.clip(jnp.exp(jax.random.uniform(key_of[3], (3, 2 * R + 1), jnp.float32, math.log(0.05), math.log(1.0))), 0.05, 1.0),
    }


def band_table(weights, count_in, count_out, offset):
    source = jnp.arange(count_in, dtype=jnp.int32)[:, None]
    target = jnp.arange(count_out, dtype=jnp.int32)[None, :]
    spread = source - target + offset
    table = jnp.zeros((count_in, count_out), jnp.float32)
    for place in range(weights.shape[0]):
        table = table + jnp.where(spread == place, weights[place], jnp.float32(0.0))
    return table


def blur(volume, kernels):
    padded_x = jnp.pad(volume, ((0, 0), (0, 0), (R, R)))
    along_x = jnp.zeros_like(volume)
    for tap_index in range(2 * R + 1):
        along_x = along_x + kernels[2, tap_index] * padded_x[:, :, tap_index:tap_index + NX]
    table_y = band_table(kernels[1], NY, NY, R)
    along_y = jnp.einsum("zyx,yw->zwx", along_x, table_y, precision=lax.Precision.HIGHEST)
    padded = jnp.pad(along_y, ((R, R), (0, 0), (0, 0)))
    total = jnp.zeros_like(along_y)
    for tap_index in range(2 * R + 1):
        total = total + kernels[0, tap_index] * padded[tap_index:tap_index + NZ]
    return total


def reference(view_a, view_b_own, spread_a, spread_b):
    view_b = jnp.transpose(view_b_own, (2, 1, 0))[:, :, ::-1]
    blur_a = spread_a / jnp.sum(spread_a, axis=1, keepdims=True)
    blur_b = spread_b / jnp.sum(spread_b, axis=1, keepdims=True)
    estimate = 0.5 * (view_a + view_b)
    for iteration in range(ITERS):
        for measured, kernels in ((view_a, blur_a), (view_b, blur_b)):
            quotient = measured / blur(estimate, kernels)
            estimate = estimate * blur(quotient, kernels[:, ::-1])
    return estimate
```

```python
import functools

import jax
import jax.numpy as jnp
from jax import lax
from jax.experimental import pallas as pl
from jax.experimental.pallas import tpu as pltpu
from jax.sharding import PartitionSpec as P

LANES = 128
QUARTERS = 4
BAND = 8


def padded(cells, sides, width):
    for axis, dim in sides:
        count = lax.axis_size(axis)
        ends = count - 1
        head = lax.slice_in_dim(cells, 0, width, axis=dim)
        tail = lax.slice_in_dim(cells, cells.shape[dim] - width, cells.shape[dim], axis=dim)
        cells = jnp.concatenate(
            [
                lax.ppermute(tail, axis, [(i, (i + 1) % count) for i in range(ends)]),
                cells,
                lax.ppermute(head, axis, [((i + 1) % count, i) for i in range(ends)]),
            ],
            axis=dim,
        )
    return cells


def band_table(weights, count_in, count_out, offset):
    source = jnp.arange(count_in, dtype=jnp.int32)[:, None]
    target = jnp.arange(count_out, dtype=jnp.int32)[None, :]
    spread = source - target + offset
    table = jnp.zeros((count_in, count_out), jnp.float32)
    for place in range(weights.shape[0]):
        table = table + jnp.where(spread == place, weights[place], jnp.float32(0.0))
    return table


def blur(volume, kernels):
    count_z, count_y, count_x = volume.shape
    radius = (kernels.shape[1] - 1) // 2
    table_x = band_table(kernels[2], count_x, count_x, radius)
    along_x = jnp.einsum("zyx,xw->zyw", volume, table_x, precision=lax.Precision.HIGHEST)
    table_y = band_table(kernels[1], count_y + 2 * radius, count_y, 0)
    widened = padded(along_x, (("gy", 1),), radius)
    narrow_y = jnp.einsum("zyx,yw->zwx", widened, table_y, precision=lax.Precision.HIGHEST)
    along_y = padded(narrow_y, (("gz", 0),), radius)
    table_z = band_table(kernels[0], count_z + 2 * radius, count_z, 0)
    return jnp.einsum("zyx,zw->wyx", along_y, table_z, precision=lax.Precision.HIGHEST)


def shards(view_a, view_b_own, spread_a, spread_b):
    arrived = lax.all_to_all(view_b_own, "gz", split_axis=2, concat_axis=0, tiled=True)
    view_b = jnp.transpose(arrived, (2, 1, 0))[:, :, ::-1]
    blur_a = spread_a / jnp.sum(spread_a, axis=1, keepdims=True)
    blur_b = spread_b / jnp.sum(spread_b, axis=1, keepdims=True)
    estimate = 0.5 * (view_a + view_b)
    for measured, kernels in ((view_a, blur_a), (view_b, blur_b)):
        quotient = measured / blur(estimate, kernels)
        estimate = estimate * blur(quotient, kernels[:, ::-1])
    return estimate


def block_transpose(parts, width):
    lane = lax.broadcasted_iota(jnp.int32, parts[0].shape, 1)
    for step in (2, 1):
        shift = step * width
        low = lax.rem(lane // shift, 2) == 0
        out = list(parts)
        for first in range(QUARTERS):
            if first & step:
                continue
            second = first + step
            out[first] = jnp.where(low, parts[first], pltpu.roll(parts[second], shift, 1))
            out[second] = jnp.where(low, pltpu.roll(parts[first], LANES - shift, 1), parts[second])
        parts = out
    return parts


def split(values):
    high = values.astype(jnp.bfloat16)
    return high, (values - high.astype(jnp.float32)).astype(jnp.bfloat16)


def dot(a, b):
    return jnp.dot(a, b, preferred_element_type=jnp.float32)


def deconvolve(
    va_hbm, vb_hbm, sa_hbm, sb_hbm, out_ref,
    va_ref, vb_ref, sa_ref, sb_ref,
    send_a, recv_a, recv_b, view_a, view_b, estimate, blurred, wide_x,
    send_e, recv_e, tz_high, tz_low, ty_high, ty_low,
    in_sem, a_send_sem, a_recv_sem, b_sem, h_send_sem, h_recv_sem, e_send_sem, e_recv_sem,
):
    f32 = jnp.float32
    groups = lax.axis_size("gz")
    devices = 2 * groups
    block = lax.axis_index("blocks")
    gz, gy = lax.axis_index("gz"), lax.axis_index("gy")
    me = 2 * gz + gy
    slab = 2 * (groups - 1 - gz) + gy
    deep, tall, long_x = va_ref.shape
    wide, full_y, full_z = view_a.shape
    taps = sa_ref.shape[1]
    radius = (taps - 1) // 2
    rows_y = tall // QUARTERS
    bands = full_y // BAND
    side_bands = tall // BAND
    lines = BAND // QUARTERS
    order = [side * side_bands + half for half in range(side_bands) for side in range(2)]
    spreads = (sa_ref, sb_ref)

    def slab_of(device):
        return 2 * (groups - 1 - device // 2) + lax.rem(device, 2)

    def at(device):
        return (block, device // 2, lax.rem(device, 2))

    def device_of(place):
        return (block, groups - 1 - place // 2, lax.rem(place, 2))

    def remote(src, dst, send_sem, recv_sem, device):
        return pltpu.make_async_remote_copy(
            src_ref=src, dst_ref=dst, send_sem=send_sem, recv_sem=recv_sem,
            device_id=device, device_id_type=pl.DeviceIdType.MESH,
        )

    loads = [
        pltpu.make_async_copy(src, dst, in_sem.at[index])
        for index, (src, dst) in enumerate(
            ((va_hbm, va_ref), (vb_hbm, vb_ref), (sa_hbm, sa_ref), (sb_hbm, sb_ref))
        )
    ]
    for load in loads:
        load.start()
    barrier = pltpu.get_barrier_semaphore()
    for hop in range(1, devices):
        pl.semaphore_signal(
            barrier, inc=1, device_id=at(lax.rem(me + hop, devices)), device_id_type=pl.DeviceIdType.MESH
        )

    loads[0].wait()
    for y in range(rows_y):
        for column in range(long_x // LANES):
            pieces = [
                va_ref[:, QUARTERS * y + q, column * LANES:(column + 1) * LANES] for q in range(QUARTERS)
            ]
            for k, piece in enumerate(block_transpose(pieces, wide)):
                send_a[QUARTERS * column + k, y] = piece

    loads[1].wait()
    pl.semaphore_wait(barrier, devices - 1)

    half = remote(
        vb_ref.at[pl.ds(wide * gy, wide)], recv_b, b_sem.at[0], b_sem.at[1], (block, gz, 1 - gy)
    )
    half.start()
    own_z = pl.ds(pl.multiple_of(gz * deep, 8), deep)

    def copy_a(part, hop):
        target = lax.rem(me + hop, devices)
        rows = pl.ds(lines * part, lines)
        return remote(
            send_a.at[slab_of(target), rows], recv_a.at[gy, rows, own_z],
            a_send_sem.at[part, hop], a_recv_sem.at[part, hop], at(target),
        )

    for part in range(side_bands):
        for hop in range(1, devices):
            copy_a(part, hop).start()
    recv_a[gy, :, own_z] = send_a[slab]

    loads[2].wait()
    loads[3].wait()
    row = lax.broadcasted_iota(jnp.int32, (full_z, LANES), 0)
    col = lax.broadcasted_iota(jnp.int32, (full_z, LANES), 1)
    for which, spread in enumerate(spreads):
        total = f32(1.0)
        for axis in range(3):
            line = spread[axis, 0]
            for tap in range(1, taps):
                line = line + spread[axis, tap]
            total = total * line
        for flipped in range(2):
            index = 2 * which + flipped
            sign = -1 if flipped else 1
            offset = sign * (row - col) + radius
            table = jnp.zeros((full_z, LANES), f32)
            for tap in range(taps):
                table = jnp.where(offset == tap, spread[0, tap], table)
            table = table / jnp.full((full_z, LANES), total, f32)
            tz_high[index], tz_low[index] = split(table)
            offset = jnp.where(row // full_y == col // full_y, sign * (col - row) + radius, -1)
            table = jnp.zeros((LANES, LANES), f32)
            for tap in range(taps):
                table = jnp.where(offset == tap, spread[1, tap], table)
            ty_high[index], ty_low[index] = split(table)

    mine, other = pl.multiple_of(gy * tall, 8), pl.multiple_of((1 - gy) * tall, 8)
    for x in range(wide):
        view_b[x, pl.ds(mine, tall)] = vb_ref[2 * wide - 1 - wide * gy - x]
    half.wait()
    for x in range(wide):
        view_b[x, pl.ds(other, tall)] = recv_b[wide - 1 - x]

    outer = jnp.where(gy == 0, slab > 0, slab < devices - 1)
    neighbour = device_of(jnp.clip(slab + 2 * gy - 1, 0, devices - 1))

    @pl.when(jnp.logical_not(outer))
    def _():
        for turn in range(4):
            wide_x[turn, pl.ds((radius + wide) * gy, radius)] = jnp.zeros((radius, full_y, full_z), f32)

    def halo(turn, band, inner):
        ys = pl.ds(band * BAND, BAND) if isinstance(band, int) else pl.ds(pl.multiple_of(band * BAND, BAND), BAND)
        source = radius + (wide - radius) * ((1 - gy) if inner else gy)
        target = (radius + wide) * (gy if inner else (1 - gy))
        return remote(
            wide_x.at[turn, pl.ds(source, radius), ys], wide_x.at[turn, pl.ds(target, radius), ys],
            h_send_sem.at[turn, band, inner], h_recv_sem.at[turn, band, inner],
            (block, gz, 1 - gy) if inner else neighbour,
        )

    def send_outer(turn, band):
        pl.when(outer)(halo(turn, band, 0).start)

    def send_inner(turn, band):
        halo(turn, band, 1).start()

    def await_halos(turn, band):
        halo(turn, band, 1).wait_recv()
        pl.when(outer)(halo(turn, band, 0).wait_recv)

    def x_taps(turn, which, flipped, band, edges, finish):
        ys = pl.ds(band * BAND, BAND) if isinstance(band, int) else pl.ds(pl.multiple_of(band * BAND, BAND), BAND)
        spread = spreads[which]
        weights = [spread[2, taps - 1 - tap if flipped else tap] for tap in range(taps)]
        for x in range(wide):
            total = blurred[x, ys] if edges else None
            for tap in range(taps):
                place = x + tap
                if (radius <= place < radius + wide) != edges:
                    term = weights[tap] * wide_x[turn, place, ys]
                    total = term if total is None else total + term
            finish(x, ys, total)

    def keep(x, ys, total):
        blurred[x, ys] = total

    for part in range(side_bands):
        for hop in range(1, devices):
            copy_a(part, hop).wait_recv()
        for side in range(2):
            for y in range(lines * part, lines * (part + 1)):
                turned = recv_a[side, y].T
                for q in range(QUARTERS):
                    view_a[:, side * tall + QUARTERS * y + q, :] = turned[q * wide:(q + 1) * wide]
        for side in range(2):
            band = side * side_bands + part
            ys = pl.ds(band * BAND, BAND)
            start = 0.5 * (view_a[:, ys] + view_b[:, ys])
            estimate[:, ys] = start
            wide_x[0, pl.ds(radius, wide), ys] = start
            send_outer(0, band)
            send_inner(0, band)

    planes = LANES // full_y
    chunks = wide // planes // 2

    def along_zy(values, index):
        high, low = split(values.reshape(chunks * LANES, full_z))
        zh = tz_high[index]
        done = dot(high, zh) + (dot(low, zh) + dot(high, tz_low[index]))
        high, low = split(done)
        yh, yl = ty_high[index], ty_low[index]
        outs = []
        for chunk in range(chunks):
            rows = slice(chunk * LANES, (chunk + 1) * LANES)
            outs.append(dot(yh, high[rows]) + (dot(yh, low[rows]) + dot(yl, high[rows])))
        return jnp.concatenate(outs, axis=0).reshape(wide // 2, full_y, full_z)

    def middle(turn, which, view):
        for step in range(2):
            first = (wide // 2) * (gy if step == 0 else 1 - gy)
            span = pl.ds(first, wide // 2)
            quotient = view[span] / along_zy(blurred[span], 2 * which)
            wide_x[turn, pl.ds(radius + first, wide // 2)] = along_zy(quotient, 2 * which + 1)
            for band in order:
                (send_inner if step else send_outer)(turn, band)

    def looped(body):
        def step(index, carry):
            body(lax.rem(index, 2) * side_bands + index // 2)
            return carry

        lax.fori_loop(0, bands, step, 0)

    looped(lambda band: x_taps(0, 0, 0, band, False, keep))

    def first_edges(band):
        await_halos(0, band)
        x_taps(0, 0, 0, band, True, keep)

    looped(first_edges)
    middle(1, 0, view_a)
    looped(lambda band: x_taps(1, 0, 1, band, False, keep))

    def update(x, ys, total):
        value = estimate[x, ys] * total
        estimate[x, ys] = value
        wide_x[2, radius + x, ys] = value

    def second_edges(band):
        await_halos(1, band)
        x_taps(1, 0, 1, band, True, update)
        send_outer(2, band)
        send_inner(2, band)
        x_taps(2, 1, 0, band, False, keep)

    looped(second_edges)

    def third_edges(band):
        await_halos(2, band)
        x_taps(2, 1, 0, band, True, keep)

    looped(third_edges)
    middle(3, 1, view_b)
    looped(lambda band: x_taps(3, 1, 1, band, False, keep))

    def last(x, ys, total):
        estimate[x, ys] = estimate[x, ys] * total

    def copy_e(side, part, step):
        target = 2 * lax.rem(gz + step, groups) + side
        hop = lax.rem(target - me + devices, devices)
        rows = pl.ds(lines * part, lines)
        return remote(
            send_e.at[side, rows, pl.ds(pl.multiple_of(target // 2 * deep, 8), deep)], recv_e.at[slab, rows],
            e_send_sem.at[part, hop], e_recv_sem.at[part, hop], at(target),
        )

    for band in order:
        side, part = band // side_bands, band % side_bands
        await_halos(3, band)
        x_taps(3, 1, 1, band, True, last)
        for y in range(lines * part, lines * (part + 1)):
            strips = [estimate[:, side * tall + QUARTERS * y + q, :] for q in range(QUARTERS)]
            send_e[side, y] = jnp.concatenate(strips, axis=0).T
        for step in range(1, groups):
            copy_e(side, part, step).start()
        pl.when(gy != side)(copy_e(side, part, 0).start)

    recv_e[slab] = send_e[gy, :, own_z]
    for part in range(side_bands):
        for hop in range(1, devices):
            remote(
                send_e.at[0, pl.ds(0, lines), pl.ds(0, deep)], recv_e.at[slab, pl.ds(lines * part, lines)],
                e_send_sem.at[part, hop], e_recv_sem.at[part, hop], at(lax.rem(me + hop, devices)),
            ).wait_recv()
        for y in range(lines * part, lines * (part + 1)):
            for column in range(long_x // LANES):
                pieces = [recv_e[QUARTERS * column + k, y] for k in range(QUARTERS)]
                for q, piece in enumerate(block_transpose(pieces, wide)):
                    out_ref[QUARTERS * y + q, :, column * LANES:(column + 1) * LANES] = piece

    for part in range(side_bands):
        for hop in range(1, devices):
            copy_a(part, hop).wait_send()
        for side in range(2):
            for step in range(1, groups):
                copy_e(side, part, step).wait_send()
            pl.when(gy != side)(copy_e(side, part, 0).wait_send)
    for turn in range(4):
        for band in range(bands):
            halo(turn, band, 1).wait_send()
            pl.when(outer)(halo(turn, band, 0).wait_send)


def slab_shards(view_a, view_b_own, spread_a, spread_b):
    groups = lax.axis_size("gz")
    deep, tall, long_x = view_a.shape
    devices = 2 * groups
    wide = long_x // devices
    full_y, full_z = 2 * tall, view_b_own.shape[2]
    taps = spread_a.shape[1]
    radius = (taps - 1) // 2
    f32, bf16 = jnp.float32, jnp.bfloat16
    volume = pltpu.VMEM((wide, full_y, full_z), f32)
    rows_y = tall // QUARTERS
    bands, halves = full_y // BAND, tall // BAND
    dma = pltpu.SemaphoreType.DMA
    turned = pl.pallas_call(
        deconvolve,
        out_shape=jax.ShapeDtypeStruct((tall, deep, long_x), f32),
        in_specs=[pl.BlockSpec(memory_space=pl.ANY)] * 4,
        out_specs=pl.BlockSpec(memory_space=pltpu.VMEM),
        scratch_shapes=[
            pltpu.VMEM(view_a.shape, f32), pltpu.VMEM(view_b_own.shape, f32),
            pltpu.SMEM(spread_a.shape, f32), pltpu.SMEM(spread_b.shape, f32),
            pltpu.VMEM((devices, rows_y, deep, LANES), f32),
            pltpu.VMEM((2, rows_y, full_z, LANES), f32),
            pltpu.VMEM((wide, tall, full_z), f32),
            volume, volume, volume, volume,
            pltpu.VMEM((4, wide + 2 * radius, full_y, full_z), f32),
            pltpu.VMEM((2, rows_y, full_z, LANES), f32),
            pltpu.VMEM((devices, rows_y, deep, LANES), f32),
            pltpu.VMEM((4, full_z, full_z), bf16), pltpu.VMEM((4, full_z, full_z), bf16),
            pltpu.VMEM((4, LANES, LANES), bf16), pltpu.VMEM((4, LANES, LANES), bf16),
            dma((4,)), dma((halves, devices)), dma((halves, devices)), dma((2,)),
            dma((4, bands, 2)), dma((4, bands, 2)), dma((halves, devices)), dma((halves, devices)),
        ],
        compiler_params=pltpu.CompilerParams(
            collective_id=0, has_side_effects=True, vmem_limit_bytes=48 * 1024 * 1024
        ),
    )(view_a, view_b_own, spread_a, spread_b)
    return jnp.transpose(turned, (1, 0, 2))


def fits_slabs(mesh, view_a, view_b_own, spread_a):
    groups, sides = mesh.shape["gz"], mesh.shape["gy"]
    deep = view_a[0] // (mesh.shape["blocks"] * groups)
    tall, wide = view_a[1] // sides, view_a[2] // (2 * groups)
    return (
        sides == 2 and wide * QUARTERS == LANES and view_b_own[2] == LANES and 4 * view_a[1] == LANES
        and tall % (8 * sides) == 0 and deep % 8 == 0 and spread_a[1] % 2 == 1 and spread_a[1] // 2 <= wide // 2
    )


def solution(mesh):
    in_specs = (P(("blocks", "gz"), "gy", None), P(("blocks", "gz"), "gy", None), P(), P())
    out_specs = P(("blocks", "gz"), "gy", None)

    def run(view_a, view_b_own, spread_a, spread_b):
        plan = slab_shards if fits_slabs(mesh, view_a.shape, view_b_own.shape, spread_a.shape) else shards
        split_plan = jax.shard_map(plan, mesh=mesh, in_specs=in_specs, out_specs=out_specs, check_vma=False)
        return split_plan(view_a, view_b_own, spread_a, spread_b)

    return run
```

```python
import functools

import jax
import jax.numpy as jnp
from jax import lax
from jax.experimental import pallas as pl
from jax.experimental.pallas import tpu as pltpu
from jax.sharding import PartitionSpec as P

LANES = 128
QUARTERS = 4
BAND = 8


def padded(cells, sides, width):
    for axis, dim in sides:
        count = lax.axis_size(axis)
        ends = count - 1
        head = lax.slice_in_dim(cells, 0, width, axis=dim)
        tail = lax.slice_in_dim(cells, cells.shape[dim] - width, cells.shape[dim], axis=dim)
        cells = jnp.concatenate(
            [
                lax.ppermute(tail, axis, [(i, (i + 1) % count) for i in range(ends)]),
                cells,
                lax.ppermute(head, axis, [((i + 1) % count, i) for i in range(ends)]),
            ],
            axis=dim,
        )
    return cells


def band_table(weights, count_in, count_out, offset):
    source = jnp.arange(count_in, dtype=jnp.int32)[:, None]
    target = jnp.arange(count_out, dtype=jnp.int32)[None, :]
    spread = source - target + offset
    table = jnp.zeros((count_in, count_out), jnp.float32)
    for place in range(weights.shape[0]):
        table = table + jnp.where(spread == place, weights[place], jnp.float32(0.0))
    return table


def blur(volume, kernels):
    count_z, count_y, count_x = volume.shape
    radius = (kernels.shape[1] - 1) // 2
    table_x = band_table(kernels[2], count_x, count_x, radius)
    along_x = jnp.einsum("zyx,xw->zyw", volume, table_x, precision=lax.Precision.HIGHEST)
    table_y = band_table(kernels[1], count_y + 2 * radius, count_y, 0)
    widened = padded(along_x, (("gy", 1),), radius)
    narrow_y = jnp.einsum("zyx,yw->zwx", widened, table_y, precision=lax.Precision.HIGHEST)
    along_y = padded(narrow_y, (("gz", 0),), radius)
    table_z = band_table(kernels[0], count_z + 2 * radius, count_z, 0)
    return jnp.einsum("zyx,zw->wyx", along_y, table_z, precision=lax.Precision.HIGHEST)


def shards(view_a, view_b_own, spread_a, spread_b):
    arrived = lax.all_to_all(view_b_own, "gz", split_axis=2, concat_axis=0, tiled=True)
    view_b = jnp.transpose(arrived, (2, 1, 0))[:, :, ::-1]
    blur_a = spread_a / jnp.sum(spread_a, axis=1, keepdims=True)
    blur_b = spread_b / jnp.sum(spread_b, axis=1, keepdims=True)
    estimate = 0.5 * (view_a + view_b)
    for measured, kernels in ((view_a, blur_a), (view_b, blur_b)):
        quotient = measured / blur(estimate, kernels)
        estimate = estimate * blur(quotient, kernels[:, ::-1])
    return estimate


def block_transpose(parts, width):
    lane = lax.broadcasted_iota(jnp.int32, parts[0].shape, 1)
    for step in (2, 1):
        shift = step * width
        low = lax.rem(lane // shift, 2) == 0
        out = list(parts)
        for first in range(QUARTERS):
            if first & step:
                continue
            second = first + step
            out[first] = jnp.where(low, parts[first], pltpu.roll(parts[second], shift, 1))
            out[second] = jnp.where(low, pltpu.roll(parts[first], LANES - shift, 1), parts[second])
        parts = out
    return parts


def split(values):
    high = values.astype(jnp.bfloat16)
    return high, (values - high.astype(jnp.float32)).astype(jnp.bfloat16)


def dot(a, b):
    return jnp.dot(a, b, preferred_element_type=jnp.float32)


def deconvolve(
    va_hbm, vb_hbm, sa_hbm, sb_hbm, out_ref,
    va_ref, vb_ref, sa_ref, sb_ref,
    send_a, recv_a, recv_b, relay, view_a, view_b, estimate, blurred, wide_x,
    send_e, recv_e, tz_high, tz_low, ty_high, ty_low,
    in_sem, a_send_sem, a_recv_sem, b_send_sem, b_recv_sem, r_send_sem, r_recv_sem, h_send_sem, h_recv_sem, e_send_sem, e_recv_sem,
):
    f32 = jnp.float32
    groups = lax.axis_size("gz")
    devices = 2 * groups
    block = lax.axis_index("blocks")
    gz, gy = lax.axis_index("gz"), lax.axis_index("gy")
    me = 2 * gz + gy
    deep, tall, long_x = va_ref.shape
    wide, full_y, full_z = view_a.shape
    taps = sa_ref.shape[1]
    radius = (taps - 1) // 2
    rows_y = tall // QUARTERS
    bands = full_y // BAND
    side_bands = tall // BAND
    lines = BAND // QUARTERS
    order = [side * side_bands + half for half in range(side_bands) for side in range(2)]
    spreads = (sa_ref, sb_ref)
    mirror = gz + 1 - 2 * lax.rem(gz, 2)
    crossed = lax.rem(gz // 2 + block, 2) == 1
    direct_x = wide // 2

    def snake(group):
        return jnp.where(lax.rem(group // 2 + block, 2) == 1, group + 1 - 2 * lax.rem(group, 2), group)

    def slab_of(device):
        return 2 * (groups - 1 - snake(device // 2)) + lax.rem(device, 2)

    def at(device):
        return (block, device // 2, lax.rem(device, 2))

    def device_of(place):
        return (block, snake(groups - 1 - place // 2), lax.rem(place, 2))

    slab = slab_of(me)

    def remote(src, dst, send_sem, recv_sem, device):
        return pltpu.make_async_remote_copy(
            src_ref=src, dst_ref=dst, send_sem=send_sem, recv_sem=recv_sem,
            device_id=device, device_id_type=pl.DeviceIdType.MESH,
        )

    loads = [
        pltpu.make_async_copy(src, dst, in_sem.at[index])
        for index, (src, dst) in enumerate(
            ((va_hbm, va_ref), (vb_hbm, vb_ref), (sa_hbm, sa_ref), (sb_hbm, sb_ref))
        )
    ]
    for load in loads:
        load.start()
    barrier = pltpu.get_barrier_semaphore()
    for hop in range(1, devices):
        pl.semaphore_signal(
            barrier, inc=1, device_id=at(lax.rem(me + hop, devices)), device_id_type=pl.DeviceIdType.MESH
        )

    for group, core in ((gz, gy), (mirror, 0), (mirror, 1)):
        pl.semaphore_signal(
            barrier, inc=1, device_id=(1 - block, group, core), device_id_type=pl.DeviceIdType.MESH
        )

    loads[0].wait()
    for y in range(rows_y):
        for column in range(long_x // LANES):
            pieces = [
                va_ref[:, QUARTERS * y + q, column * LANES:(column + 1) * LANES] for q in range(QUARTERS)
            ]
            for k, piece in enumerate(block_transpose(pieces, wide)):
                send_a[QUARTERS * column + k, y] = piece

    loads[1].wait()
    pl.semaphore_wait(barrier, devices + 2)

    half = remote(
        vb_ref.at[pl.ds(wide * gy, wide)], recv_b.at[gy], b_send_sem.at[0, 0], b_recv_sem.at[gy, 0], (block, gz, 1 - gy)
    )

    def direct(core):
        return remote(
            vb_ref.at[pl.ds(wide * (1 - core), direct_x)], recv_b.at[gy, pl.ds(0, direct_x)],
            b_send_sem.at[core, 0], b_recv_sem.at[gy, 0], (block, mirror, core),
        )

    def detour(core):
        return remote(
            vb_ref.at[pl.ds(wide * (1 - core) + direct_x, wide - direct_x)], relay.at[core],
            b_send_sem.at[core, 1], r_recv_sem.at[core], (1 - block, gz, gy),
        )

    def onward(core):
        return remote(
            relay.at[core], recv_b.at[gy, pl.ds(direct_x, wide - direct_x)],
            r_send_sem.at[core], b_recv_sem.at[gy, 1], (1 - block, mirror, core),
        )

    @pl.when(crossed)
    def _():
        for core in range(2):
            detour(core).start()

    pl.when(jnp.logical_not(crossed))(half.start)
    own_z = pl.ds(pl.multiple_of(gz * deep, 8), deep)

    def copy_a(part, hop):
        target = lax.rem(me + hop, devices)
        rows = pl.ds(lines * part, lines)
        return remote(
            send_a.at[slab_of(target), rows], recv_a.at[gy, rows, own_z],
            a_send_sem.at[part, hop], a_recv_sem.at[part, hop], at(target),
        )

    for part in range(side_bands):
        for hop in range(1, devices):
            copy_a(part, hop).start()
    recv_a[gy, :, own_z] = send_a[slab]

    @pl.when(crossed)
    def _():
        for core in range(2):
            direct(core).start()


    loads[2].wait()
    loads[3].wait()
    row = lax.broadcasted_iota(jnp.int32, (full_z, LANES), 0)
    col = lax.broadcasted_iota(jnp.int32, (full_z, LANES), 1)
    for which, spread in enumerate(spreads):
        total = f32(1.0)
        for axis in range(3):
            line = spread[axis, 0]
            for tap in range(1, taps):
                line = line + spread[axis, tap]
            total = total * line
        for flipped in range(2):
            index = 2 * which + flipped
            sign = -1 if flipped else 1
            offset = sign * (row - col) + radius
            table = jnp.zeros((full_z, LANES), f32)
            for tap in range(taps):
                table = jnp.where(offset == tap, spread[0, tap], table)
            table = table / jnp.full((full_z, LANES), total, f32)
            tz_high[index], tz_low[index] = split(table)
            offset = jnp.where(row // full_y == col // full_y, sign * (col - row) + radius, -1)
            table = jnp.zeros((LANES, LANES), f32)
            for tap in range(taps):
                table = jnp.where(offset == tap, spread[1, tap], table)
            ty_high[index], ty_low[index] = split(table)

    mine, other = pl.multiple_of(gy * tall, 8), pl.multiple_of((1 - gy) * tall, 8)

    @pl.when(jnp.logical_not(crossed))
    def _():
        for core in range(2):
            detour(core).wait_recv()
            onward(core).start()
        for x in range(wide):
            view_b[x, pl.ds(mine, tall)] = vb_ref[2 * wide - 1 - wide * gy - x]
        remote(
            vb_ref.at[pl.ds(0, wide)], recv_b.at[0], b_send_sem.at[0, 0], b_recv_sem.at[1 - gy, 0], (block, gz, 1 - gy)
        ).wait_recv()

    @pl.when(crossed)
    def _():
        for core in range(2):
            remote(
                vb_ref.at[pl.ds(0, direct_x)], recv_b.at[core, pl.ds(0, direct_x)],
                b_send_sem.at[0, 0], b_recv_sem.at[core, 0], (block, mirror, core),
            ).wait_recv()
            remote(
                relay.at[0], recv_b.at[core, pl.ds(direct_x, wide - direct_x)],
                r_send_sem.at[0], b_recv_sem.at[core, 1], (1 - block, mirror, core),
            ).wait_recv()
        for x in range(wide):
            view_b[x, pl.ds(mine, tall)] = recv_b[gy, wide - 1 - x]

    for x in range(wide):
        view_b[x, pl.ds(other, tall)] = recv_b[1 - gy, wide - 1 - x]

    outer = jnp.where(gy == 0, slab > 0, slab < devices - 1)
    neighbour = device_of(jnp.clip(slab + 2 * gy - 1, 0, devices - 1))

    @pl.when(jnp.logical_not(outer))
    def _():
        for turn in range(4):
            wide_x[turn, pl.ds((radius + wide) * gy, radius)] = jnp.zeros((radius, full_y, full_z), f32)

    def halo(turn, band, inner):
        ys = pl.ds(band * BAND, BAND) if isinstance(band, int) else pl.ds(pl.multiple_of(band * BAND, BAND), BAND)
        source = radius + (wide - radius) * ((1 - gy) if inner else gy)
        target = (radius + wide) * (gy if inner else (1 - gy))
        return remote(
            wide_x.at[turn, pl.ds(source, radius), ys], wide_x.at[turn, pl.ds(target, radius), ys],
            h_send_sem.at[turn, band, inner], h_recv_sem.at[turn, band, inner],
            (block, gz, 1 - gy) if inner else neighbour,
        )

    def send_outer(turn, band):
        pl.when(outer)(halo(turn, band, 0).start)

    def send_inner(turn, band):
        halo(turn, band, 1).start()

    def await_halos(turn, band):
        halo(turn, band, 1).wait_recv()
        pl.when(outer)(halo(turn, band, 0).wait_recv)

    def x_taps(turn, which, flipped, band, edges, finish):
        ys = pl.ds(band * BAND, BAND) if isinstance(band, int) else pl.ds(pl.multiple_of(band * BAND, BAND), BAND)
        spread = spreads[which]
        weights = [spread[2, taps - 1 - tap if flipped else tap] for tap in range(taps)]
        for x in range(wide):
            total = blurred[x, ys] if edges else None
            for tap in range(taps):
                place = x + tap
                if (radius <= place < radius + wide) != edges:
                    term = weights[tap] * wide_x[turn, place, ys]
                    total = term if total is None else total + term
            finish(x, ys, total)

    def keep(x, ys, total):
        blurred[x, ys] = total

    for part in range(side_bands):
        for hop in range(1, devices):
            copy_a(part, hop).wait_recv()
        for side in range(2):
            for y in range(lines * part, lines * (part + 1)):
                turned = recv_a[side, y].T
                for q in range(QUARTERS):
                    view_a[:, side * tall + QUARTERS * y + q, :] = turned[q * wide:(q + 1) * wide]
        for side in range(2):
            band = side * side_bands + part
            ys = pl.ds(band * BAND, BAND)
            start = 0.5 * (view_a[:, ys] + view_b[:, ys])
            estimate[:, ys] = start
            wide_x[0, pl.ds(radius, wide), ys] = start
            send_outer(0, band)
            send_inner(0, band)

    planes = LANES // full_y
    chunks = wide // planes // 2

    def along_zy(values, index):
        high, low = split(values.reshape(chunks * LANES, full_z))
        zh = tz_high[index]
        done = dot(high, zh) + (dot(low, zh) + dot(high, tz_low[index]))
        high, low = split(done)
        yh, yl = ty_high[index], ty_low[index]
        outs = []
        for chunk in range(chunks):
            rows = slice(chunk * LANES, (chunk + 1) * LANES)
            outs.append(dot(yh, high[rows]) + (dot(yh, low[rows]) + dot(yl, high[rows])))
        return jnp.concatenate(outs, axis=0).reshape(wide // 2, full_y, full_z)

    def middle(turn, which, view):
        for step in range(2):
            first = (wide // 2) * (gy if step == 0 else 1 - gy)
            span = pl.ds(first, wide // 2)
            quotient = view[span] / along_zy(blurred[span], 2 * which)
            wide_x[turn, pl.ds(radius + first, wide // 2)] = along_zy(quotient, 2 * which + 1)
            for band in order:
                (send_inner if step else send_outer)(turn, band)

    def looped(body):
        def step(index, carry):
            body(lax.rem(index, 2) * side_bands + index // 2)
            return carry

        lax.fori_loop(0, bands, step, 0)

    looped(lambda band: x_taps(0, 0, 0, band, False, keep))

    def first_edges(band):
        await_halos(0, band)
        x_taps(0, 0, 0, band, True, keep)

    looped(first_edges)
    middle(1, 0, view_a)
    looped(lambda band: x_taps(1, 0, 1, band, False, keep))

    def update(x, ys, total):
        value = estimate[x, ys] * total
        estimate[x, ys] = value
        wide_x[2, radius + x, ys] = value

    def second_edges(band):
        await_halos(1, band)
        x_taps(1, 0, 1, band, True, update)
        send_outer(2, band)
        send_inner(2, band)
        x_taps(2, 1, 0, band, False, keep)

    looped(second_edges)

    def third_edges(band):
        await_halos(2, band)
        x_taps(2, 1, 0, band, True, keep)

    looped(third_edges)
    middle(3, 1, view_b)
    looped(lambda band: x_taps(3, 1, 1, band, False, keep))

    def last(x, ys, total):
        estimate[x, ys] = estimate[x, ys] * total

    def copy_e(side, part, step):
        target = 2 * lax.rem(gz + step, groups) + side
        hop = lax.rem(target - me + devices, devices)
        rows = pl.ds(lines * part, lines)
        return remote(
            send_e.at[side, rows, pl.ds(pl.multiple_of(target // 2 * deep, 8), deep)], recv_e.at[slab, rows],
            e_send_sem.at[part, hop], e_recv_sem.at[part, hop], at(target),
        )

    for band in order:
        side, part = band // side_bands, band % side_bands
        await_halos(3, band)
        x_taps(3, 1, 1, band, True, last)
        for y in range(lines * part, lines * (part + 1)):
            strips = [estimate[:, side * tall + QUARTERS * y + q, :] for q in range(QUARTERS)]
            send_e[side, y] = jnp.concatenate(strips, axis=0).T
        for step in range(1, groups):
            copy_e(side, part, step).start()
        pl.when(gy != side)(copy_e(side, part, 0).start)

    recv_e[slab] = send_e[gy, :, own_z]
    for part in range(side_bands):
        for hop in range(1, devices):
            remote(
                send_e.at[0, pl.ds(0, lines), pl.ds(0, deep)], recv_e.at[slab, pl.ds(lines * part, lines)],
                e_send_sem.at[part, hop], e_recv_sem.at[part, hop], at(lax.rem(me + hop, devices)),
            ).wait_recv()
        for y in range(lines * part, lines * (part + 1)):
            for column in range(long_x // LANES):
                pieces = [recv_e[QUARTERS * column + k, y] for k in range(QUARTERS)]
                for q, piece in enumerate(block_transpose(pieces, wide)):
                    out_ref[QUARTERS * y + q, :, column * LANES:(column + 1) * LANES] = piece

    for part in range(side_bands):
        for hop in range(1, devices):
            copy_a(part, hop).wait_send()
        for side in range(2):
            for step in range(1, groups):
                copy_e(side, part, step).wait_send()
            pl.when(gy != side)(copy_e(side, part, 0).wait_send)

    @pl.when(crossed)
    def _():
        for core in range(2):
            detour(core).wait_send()
            direct(core).wait_send()

    @pl.when(jnp.logical_not(crossed))
    def _():
        half.wait_send()
        for core in range(2):
            onward(core).wait_send()

    for turn in range(4):
        for band in range(bands):
            halo(turn, band, 1).wait_send()
            pl.when(outer)(halo(turn, band, 0).wait_send)


def slab_shards(view_a, view_b_own, spread_a, spread_b):
    groups = lax.axis_size("gz")
    deep, tall, long_x = view_a.shape
    devices = 2 * groups
    wide = long_x // devices
    full_y, full_z = 2 * tall, view_b_own.shape[2]
    taps = spread_a.shape[1]
    radius = (taps - 1) // 2
    f32, bf16 = jnp.float32, jnp.bfloat16
    volume = pltpu.VMEM((wide, full_y, full_z), f32)
    rows_y = tall // QUARTERS
    bands, halves = full_y // BAND, tall // BAND
    dma = pltpu.SemaphoreType.DMA
    turned = pl.pallas_call(
        deconvolve,
        out_shape=jax.ShapeDtypeStruct((tall, deep, long_x), f32),
        in_specs=[pl.BlockSpec(memory_space=pl.ANY)] * 4,
        out_specs=pl.BlockSpec(memory_space=pltpu.VMEM),
        scratch_shapes=[
            pltpu.VMEM(view_a.shape, f32), pltpu.VMEM(view_b_own.shape, f32),
            pltpu.SMEM(spread_a.shape, f32), pltpu.SMEM(spread_b.shape, f32),
            pltpu.VMEM((devices, rows_y, deep, LANES), f32),
            pltpu.VMEM((2, rows_y, full_z, LANES), f32),
            pltpu.VMEM((2, wide, tall, full_z), f32),
            pltpu.VMEM((2, wide // 2, tall, full_z), f32),
            volume, volume, volume, volume,
            pltpu.VMEM((4, wide + 2 * radius, full_y, full_z), f32),
            pltpu.VMEM((2, rows_y, full_z, LANES), f32),
            pltpu.VMEM((devices, rows_y, deep, LANES), f32),
            pltpu.VMEM((4, full_z, full_z), bf16), pltpu.VMEM((4, full_z, full_z), bf16),
            pltpu.VMEM((4, LANES, LANES), bf16), pltpu.VMEM((4, LANES, LANES), bf16),
            dma((4,)), dma((halves, devices)), dma((halves, devices)), dma((2, 2)), dma((2, 2)), dma((2,)), dma((2,)),
            dma((4, bands, 2)), dma((4, bands, 2)), dma((halves, devices)), dma((halves, devices)),
        ],
        compiler_params=pltpu.CompilerParams(
            collective_id=0, has_side_effects=True, vmem_limit_bytes=56000000
        ),
    )(view_a, view_b_own, spread_a, spread_b)
    return jnp.transpose(turned, (1, 0, 2))


def fits_slabs(mesh, view_a, view_b_own, spread_a):
    groups, sides = mesh.shape["gz"], mesh.shape["gy"]
    deep = view_a[0] // (mesh.shape["blocks"] * groups)
    tall, wide = view_a[1] // sides, view_a[2] // (2 * groups)
    return (
        mesh.shape["blocks"] == 2 and groups % 2 == 0 and sides == 2 and wide * QUARTERS == LANES and view_b_own[2] == LANES and 4 * view_a[1] == LANES
        and tall % (8 * sides) == 0 and deep % 8 == 0 and spread_a[1] % 2 == 1 and spread_a[1] // 2 <= wide // 2
    )


def solution(mesh):
    in_specs = (P(("blocks", "gz"), "gy", None), P(("blocks", "gz"), "gy", None), P(), P())
    out_specs = P(("blocks", "gz"), "gy", None)

    def run(view_a, view_b_own, spread_a, spread_b):
        plan = slab_shards if fits_slabs(mesh, view_a.shape, view_b_own.shape, spread_a.shape) else shards
        split_plan = jax.shard_map(plan, mesh=mesh, in_specs=in_specs, out_specs=out_specs, check_vma=False)
        return split_plan(view_a, view_b_own, spread_a, spread_b)

    return run
```

```python
import functools

import jax
import jax.numpy as jnp
from jax import lax
from jax.experimental import pallas as pl
from jax.experimental.pallas import tpu as pltpu
from jax.sharding import PartitionSpec as P

LANES = 128
QUARTERS = 4
BAND = 8


def padded(cells, sides, width):
    for axis, dim in sides:
        count = lax.axis_size(axis)
        ends = count - 1
        head = lax.slice_in_dim(cells, 0, width, axis=dim)
        tail = lax.slice_in_dim(cells, cells.shape[dim] - width, cells.shape[dim], axis=dim)
        cells = jnp.concatenate(
            [
                lax.ppermute(tail, axis, [(i, (i + 1) % count) for i in range(ends)]),
                cells,
                lax.ppermute(head, axis, [((i + 1) % count, i) for i in range(ends)]),
            ],
            axis=dim,
        )
    return cells


def band_table(weights, count_in, count_out, offset):
    source = jnp.arange(count_in, dtype=jnp.int32)[:, None]
    target = jnp.arange(count_out, dtype=jnp.int32)[None, :]
    spread = source - target + offset
    table = jnp.zeros((count_in, count_out), jnp.float32)
    for place in range(weights.shape[0]):
        table = table + jnp.where(spread == place, weights[place], jnp.float32(0.0))
    return table


def blur(volume, kernels):
    count_z, count_y, count_x = volume.shape
    radius = (kernels.shape[1] - 1) // 2
    table_x = band_table(kernels[2], count_x, count_x, radius)
    along_x = jnp.einsum("zyx,xw->zyw", volume, table_x, precision=lax.Precision.HIGHEST)
    table_y = band_table(kernels[1], count_y + 2 * radius, count_y, 0)
    widened = padded(along_x, (("gy", 1),), radius)
    narrow_y = jnp.einsum("zyx,yw->zwx", widened, table_y, precision=lax.Precision.HIGHEST)
    along_y = padded(narrow_y, (("gz", 0),), radius)
    table_z = band_table(kernels[0], count_z + 2 * radius, count_z, 0)
    return jnp.einsum("zyx,zw->wyx", along_y, table_z, precision=lax.Precision.HIGHEST)


def shards(view_a, view_b_own, spread_a, spread_b):
    arrived = lax.all_to_all(view_b_own, "gz", split_axis=2, concat_axis=0, tiled=True)
    view_b = jnp.transpose(arrived, (2, 1, 0))[:, :, ::-1]
    blur_a = spread_a / jnp.sum(spread_a, axis=1, keepdims=True)
    blur_b = spread_b / jnp.sum(spread_b, axis=1, keepdims=True)
    estimate = 0.5 * (view_a + view_b)
    for measured, kernels in ((view_a, blur_a), (view_b, blur_b)):
        quotient = measured / blur(estimate, kernels)
        estimate = estimate * blur(quotient, kernels[:, ::-1])
    return estimate


def block_transpose(parts, width):
    lane = lax.broadcasted_iota(jnp.int32, parts[0].shape, 1)
    for step in (2, 1):
        shift = step * width
        low = lax.rem(lane // shift, 2) == 0
        out = list(parts)
        for first in range(QUARTERS):
            if first & step:
                continue
            second = first + step
            out[first] = jnp.where(low, parts[first], pltpu.roll(parts[second], shift, 1))
            out[second] = jnp.where(low, pltpu.roll(parts[first], LANES - shift, 1), parts[second])
        parts = out
    return parts


def split(values):
    high = values.astype(jnp.bfloat16)
    return high, (values - high.astype(jnp.float32)).astype(jnp.bfloat16)


def dot(a, b):
    return jnp.dot(a, b, preferred_element_type=jnp.float32)


def deconvolve(
    va_hbm, vb_hbm, sa_hbm, sb_hbm, out_ref,
    va_ref, vb_ref, sa_ref, sb_ref,
    send_a, recv_a, recv_b, relay, view_a, view_b, estimate, blurred, wide_x,
    send_e, recv_e, table_z, table_y,
    in_sem, a_send_sem, a_recv_sem, b_send_sem, b_recv_sem, r_send_sem, r_recv_sem, h_send_sem, h_recv_sem, e_send_sem, e_recv_sem,
):
    f32 = jnp.float32
    groups = lax.axis_size("gz")
    devices = 2 * groups
    block = lax.axis_index("blocks")
    gz, gy = lax.axis_index("gz"), lax.axis_index("gy")
    me = 2 * gz + gy
    deep, tall, long_x = va_ref.shape
    wide, full_y, full_z = view_a.shape
    taps = sa_ref.shape[1]
    radius = (taps - 1) // 2
    rows_y = tall // QUARTERS
    bands = full_y // BAND
    side_bands = tall // BAND
    lines = BAND // QUARTERS
    order = [side * side_bands + half for half in range(side_bands) for side in range(2)]
    spreads = (sa_ref, sb_ref)
    mirror = gz + 1 - 2 * lax.rem(gz, 2)
    crossed = lax.rem(gz // 2 + block, 2) == 1
    direct_x = wide // 2

    def snake(group):
        return jnp.where(lax.rem(group // 2 + block, 2) == 1, group + 1 - 2 * lax.rem(group, 2), group)

    def slab_of(device):
        return 2 * (groups - 1 - snake(device // 2)) + lax.rem(device, 2)

    def at(device):
        return (block, device // 2, lax.rem(device, 2))

    def device_of(place):
        return (block, snake(groups - 1 - place // 2), lax.rem(place, 2))

    slab = slab_of(me)

    def remote(src, dst, send_sem, recv_sem, device):
        return pltpu.make_async_remote_copy(
            src_ref=src, dst_ref=dst, send_sem=send_sem, recv_sem=recv_sem,
            device_id=device, device_id_type=pl.DeviceIdType.MESH,
        )

    barrier = pltpu.get_barrier_semaphore()
    for hop in range(1, devices):
        pl.semaphore_signal(
            barrier, inc=1, device_id=at(lax.rem(me + hop, devices)), device_id_type=pl.DeviceIdType.MESH
        )

    for group, core in ((gz, gy), (mirror, 0), (mirror, 1)):
        pl.semaphore_signal(
            barrier, inc=1, device_id=(1 - block, group, core), device_id_type=pl.DeviceIdType.MESH
        )

    loads = [
        pltpu.make_async_copy(src, dst, in_sem.at[index])
        for index, (src, dst) in enumerate(
            ((va_hbm, va_ref), (vb_hbm, vb_ref), (sa_hbm, sa_ref), (sb_hbm, sb_ref))
        )
    ]
    for load in loads:
        load.start()
    loads[0].wait()
    for y in range(rows_y):
        for column in range(long_x // LANES):
            pieces = [
                va_ref[:, QUARTERS * y + q, column * LANES:(column + 1) * LANES] for q in range(QUARTERS)
            ]
            for k, piece in enumerate(block_transpose(pieces, wide)):
                send_a[QUARTERS * column + k, y] = piece

    loads[1].wait()
    pl.semaphore_wait(barrier, devices + 2)

    half = remote(
        vb_ref.at[pl.ds(wide * gy, wide)], recv_b.at[gy], b_send_sem.at[0, 0, 0], b_recv_sem.at[gy, 0, 0], (block, gz, 1 - gy)
    )

    def direct(core, part):
        ys = pl.ds(BAND * part, BAND)
        return remote(
            vb_ref.at[pl.ds(wide * (1 - core), direct_x), ys], recv_b.at[gy, pl.ds(0, direct_x), ys],
            b_send_sem.at[core, 0, part], b_recv_sem.at[gy, 0, part], (block, mirror, core),
        )

    def detour(core, part):
        ys = pl.ds(BAND * part, BAND)
        return remote(
            vb_ref.at[pl.ds(wide * (1 - core) + direct_x, wide - direct_x), ys], relay.at[core, part],
            b_send_sem.at[core, 1, part], r_recv_sem.at[core, part], (1 - block, gz, gy),
        )

    def onward(core, part):
        ys = pl.ds(BAND * part, BAND)
        return remote(
            relay.at[core, part], recv_b.at[gy, pl.ds(direct_x, wide - direct_x), ys],
            r_send_sem.at[core, part], b_recv_sem.at[gy, 1, part], (1 - block, mirror, core),
        )

    @pl.when(crossed)
    def _():
        for part in range(side_bands):
            for core in range(2):
                detour(core, part).start()

    pl.when(jnp.logical_not(crossed))(half.start)
    own_z = pl.ds(pl.multiple_of(gz * deep, 8), deep)

    def copy_a(part, hop):
        target = lax.rem(me + hop, devices)
        rows = pl.ds(lines * part, lines)
        return remote(
            send_a.at[slab_of(target), rows], recv_a.at[gy, rows, own_z],
            a_send_sem.at[part, hop], a_recv_sem.at[part, hop], at(target),
        )

    for part in range(side_bands):
        for hop in range(1, devices):
            copy_a(part, hop).start()

        @pl.when(crossed)
        def _():
            for core in range(2):
                direct(core, part).start()

    recv_a[gy, :, own_z] = send_a[slab]

    loads[2].wait()
    loads[3].wait()
    row = lax.broadcasted_iota(jnp.int32, (full_z, LANES), 0)
    col = lax.broadcasted_iota(jnp.int32, (full_z, LANES), 1)
    for which, spread in enumerate(spreads):
        total = f32(1.0)
        for axis in range(3):
            line = spread[axis, 0]
            for tap in range(1, taps):
                line = line + spread[axis, tap]
            total = total * line
        for flipped in range(2):
            index = 2 * which + flipped
            sign = -1 if flipped else 1
            offset = sign * (row - col) + radius
            table = jnp.zeros((full_z, LANES), f32)
            for tap in range(taps):
                table = jnp.where(offset == tap, spread[0, tap], table)
            table = table / jnp.full((full_z, LANES), total, f32)
            high, low = split(table)
            blank = jnp.zeros((full_z, LANES), jnp.bfloat16)
            table_z[index] = jnp.concatenate(
                [jnp.concatenate([high, low], axis=1), jnp.concatenate([high, blank], axis=1)], axis=0
            )
            offset = jnp.where(row // full_y == col // full_y, sign * (col - row) + radius, -1)
            table = jnp.zeros((LANES, LANES), f32)
            for tap in range(taps):
                table = jnp.where(offset == tap, spread[1, tap], table)
            high, low = split(table)
            blank = jnp.zeros((LANES, LANES), jnp.bfloat16)
            table_y[index] = jnp.concatenate(
                [jnp.concatenate([high, high], axis=1), jnp.concatenate([low, blank], axis=1)], axis=0
            )

    mine = pl.multiple_of(gy * tall, BAND)

    @pl.when(jnp.logical_not(crossed))
    def _():
        for part in range(side_bands):
            for core in range(2):
                detour(core, part).wait_recv()
                onward(core, part).start()
        for x in range(wide):
            view_b[x, pl.ds(mine, tall)] = vb_ref[2 * wide - 1 - wide * gy - x]
        remote(
            vb_ref.at[pl.ds(0, wide)], recv_b.at[0], b_send_sem.at[0, 0, 0], b_recv_sem.at[1 - gy, 0, 0],
            (block, gz, 1 - gy),
        ).wait_recv()
        other = pl.multiple_of((1 - gy) * tall, BAND)
        for x in range(wide):
            view_b[x, pl.ds(other, tall)] = recv_b[1 - gy, wide - 1 - x]

    def crossed_view(part):
        for core in range(2):
            ys = pl.ds(BAND * part, BAND)
            remote(
                vb_ref.at[pl.ds(0, direct_x), ys], recv_b.at[core, pl.ds(0, direct_x), ys],
                b_send_sem.at[0, 0, part], b_recv_sem.at[core, 0, part], (block, mirror, core),
            ).wait_recv()
            remote(
                relay.at[0, part], recv_b.at[core, pl.ds(direct_x, wide - direct_x), ys],
                r_send_sem.at[0, part], b_recv_sem.at[core, 1, part], (1 - block, mirror, core),
            ).wait_recv()
            for x in range(wide):
                view_b[x, core * tall + BAND * part:core * tall + BAND * (part + 1)] = recv_b[core, wide - 1 - x, ys]

    outer = jnp.where(gy == 0, slab > 0, slab < devices - 1)
    neighbour = device_of(jnp.clip(slab + 2 * gy - 1, 0, devices - 1))

    @pl.when(jnp.logical_not(outer))
    def _():
        for turn in range(4):
            wide_x[turn, pl.ds((radius + wide) * gy, radius)] = jnp.zeros((radius, full_y, full_z), f32)

    def halo(turn, band, inner):
        ys = pl.ds(band * BAND, BAND) if isinstance(band, int) else pl.ds(pl.multiple_of(band * BAND, BAND), BAND)
        source = radius + (wide - radius) * ((1 - gy) if inner else gy)
        target = (radius + wide) * (gy if inner else (1 - gy))
        return remote(
            wide_x.at[turn, pl.ds(source, radius), ys], wide_x.at[turn, pl.ds(target, radius), ys],
            h_send_sem.at[turn, band, inner], h_recv_sem.at[turn, band, inner],
            (block, gz, 1 - gy) if inner else neighbour,
        )

    def send_outer(turn, band):
        pl.when(outer)(halo(turn, band, 0).start)

    def send_inner(turn, band):
        halo(turn, band, 1).start()

    def await_halos(turn, band):
        halo(turn, band, 1).wait_recv()
        pl.when(outer)(halo(turn, band, 0).wait_recv)

    def x_taps(turn, which, flipped, band, edges, finish):
        ys = pl.ds(band * BAND, BAND) if isinstance(band, int) else pl.ds(pl.multiple_of(band * BAND, BAND), BAND)
        spread = spreads[which]
        weights = [spread[2, taps - 1 - tap if flipped else tap] for tap in range(taps)]
        for x in range(wide):
            total = blurred[x, ys] if edges else None
            for tap in range(taps):
                place = x + tap
                if (radius <= place < radius + wide) != edges:
                    term = weights[tap] * wide_x[turn, place, ys]
                    total = term if total is None else total + term
            finish(x, ys, total)

    def keep(x, ys, total):
        blurred[x, ys] = total

    for part in range(side_bands):
        pl.when(crossed)(functools.partial(crossed_view, part))
        for hop in range(1, devices):
            copy_a(part, hop).wait_recv()
        for side in range(2):
            for y in range(lines * part, lines * (part + 1)):
                turned = recv_a[side, y].T
                for q in range(QUARTERS):
                    view_a[:, side * tall + QUARTERS * y + q, :] = turned[q * wide:(q + 1) * wide]
        for side in range(2):
            band = side * side_bands + part
            ys = pl.ds(band * BAND, BAND)
            start = 0.5 * (view_a[:, ys] + view_b[:, ys])
            estimate[:, ys] = start
            wide_x[0, pl.ds(radius, wide), ys] = start
            send_outer(0, band)
            send_inner(0, band)

    planes = LANES // full_y
    chunks = wide // planes // 2

    def along_zy(values, index):
        high, low = split(values.reshape(chunks * LANES, full_z))
        both = dot(jnp.concatenate([high, low], axis=1), table_z[index])
        high, low = split(both[:, :LANES] + both[:, LANES:])
        outs = []
        for chunk in range(0, chunks, 2):
            first = slice(chunk * LANES, (chunk + 1) * LANES)
            second = slice((chunk + 1) * LANES, (chunk + 2) * LANES)
            stacked = jnp.concatenate(
                [
                    jnp.concatenate([high[first], high[second]], axis=1),
                    jnp.concatenate([low[first], low[second]], axis=1),
                ],
                axis=0,
            )
            both = dot(table_y[index], stacked)
            both = both[:LANES] + both[LANES:]
            outs += [both[:, :LANES], both[:, LANES:]]
        return jnp.concatenate(outs, axis=0).reshape(wide // 2, full_y, full_z)

    def middle(turn, which, view):
        for step in range(2):
            first = (wide // 2) * (gy if step == 0 else 1 - gy)
            span = pl.ds(first, wide // 2)
            quotient = view[span] / along_zy(blurred[span], 2 * which)
            wide_x[turn, pl.ds(radius + first, wide // 2)] = along_zy(quotient, 2 * which + 1)
            for band in order:
                (send_inner if step else send_outer)(turn, band)

    def looped(body):
        def step(index, carry):
            body(lax.rem(index, 2) * side_bands + index // 2)
            return carry

        lax.fori_loop(0, bands, step, 0)

    looped(lambda band: x_taps(0, 0, 0, band, False, keep))

    def first_edges(band):
        await_halos(0, band)
        x_taps(0, 0, 0, band, True, keep)

    looped(first_edges)
    middle(1, 0, view_a)
    looped(lambda band: x_taps(1, 0, 1, band, False, keep))

    def update(x, ys, total):
        value = estimate[x, ys] * total
        estimate[x, ys] = value
        wide_x[2, radius + x, ys] = value

    def second_edges(band):
        await_halos(1, band)
        x_taps(1, 0, 1, band, True, update)
        send_outer(2, band)
        send_inner(2, band)
        x_taps(2, 1, 0, band, False, keep)

    looped(second_edges)

    def third_edges(band):
        await_halos(2, band)
        x_taps(2, 1, 0, band, True, keep)

    looped(third_edges)
    middle(3, 1, view_b)
    looped(lambda band: x_taps(3, 1, 1, band, False, keep))

    def last(x, ys, total):
        estimate[x, ys] = estimate[x, ys] * total

    def copy_e(side, part, step):
        target = 2 * lax.rem(gz + step, groups) + side
        hop = lax.rem(target - me + devices, devices)
        rows = pl.ds(lines * part, lines)
        return remote(
            send_e.at[side, rows, pl.ds(pl.multiple_of(target // 2 * deep, 8), deep)], recv_e.at[slab, rows],
            e_send_sem.at[part, hop], e_recv_sem.at[part, hop], at(target),
        )

    for band in order:
        side, part = band // side_bands, band % side_bands
        await_halos(3, band)
        x_taps(3, 1, 1, band, True, last)
        for y in range(lines * part, lines * (part + 1)):
            strips = [estimate[:, side * tall + QUARTERS * y + q, :] for q in range(QUARTERS)]
            send_e[side, y] = jnp.concatenate(strips, axis=0).T
        for step in range(1, groups):
            copy_e(side, part, step).start()
        pl.when(gy != side)(copy_e(side, part, 0).start)

    recv_e[slab] = send_e[gy, :, own_z]
    for part in range(side_bands):
        for hop in range(1, devices):
            remote(
                send_e.at[0, pl.ds(0, lines), pl.ds(0, deep)], recv_e.at[slab, pl.ds(lines * part, lines)],
                e_send_sem.at[part, hop], e_recv_sem.at[part, hop], at(lax.rem(me + hop, devices)),
            ).wait_recv()
        for y in range(lines * part, lines * (part + 1)):
            for column in range(long_x // LANES):
                pieces = [recv_e[QUARTERS * column + k, y] for k in range(QUARTERS)]
                for q, piece in enumerate(block_transpose(pieces, wide)):
                    out_ref[QUARTERS * y + q, :, column * LANES:(column + 1) * LANES] = piece

    for part in range(side_bands):
        for hop in range(1, devices):
            copy_a(part, hop).wait_send()
        for side in range(2):
            for step in range(1, groups):
                copy_e(side, part, step).wait_send()
            pl.when(gy != side)(copy_e(side, part, 0).wait_send)

    @pl.when(crossed)
    def _():
        for part in range(side_bands):
            for core in range(2):
                detour(core, part).wait_send()
                direct(core, part).wait_send()

    @pl.when(jnp.logical_not(crossed))
    def _():
        half.wait_send()
        for part in range(side_bands):
            for core in range(2):
                onward(core, part).wait_send()

    for turn in range(4):
        for band in range(bands):
            halo(turn, band, 1).wait_send()
            pl.when(outer)(halo(turn, band, 0).wait_send)


def slab_shards(view_a, view_b_own, spread_a, spread_b):
    groups = lax.axis_size("gz")
    deep, tall, long_x = view_a.shape
    devices = 2 * groups
    wide = long_x // devices
    full_y, full_z = 2 * tall, view_b_own.shape[2]
    taps = spread_a.shape[1]
    radius = (taps - 1) // 2
    f32, bf16 = jnp.float32, jnp.bfloat16
    volume = pltpu.VMEM((wide, full_y, full_z), f32)
    rows_y = tall // QUARTERS
    bands, halves = full_y // BAND, tall // BAND
    dma = pltpu.SemaphoreType.DMA
    turned = pl.pallas_call(
        deconvolve,
        out_shape=jax.ShapeDtypeStruct((tall, deep, long_x), f32),
        in_specs=[pl.BlockSpec(memory_space=pl.ANY)] * 4,
        out_specs=pl.BlockSpec(memory_space=pltpu.VMEM),
        scratch_shapes=[
            pltpu.VMEM(view_a.shape, f32), pltpu.VMEM(view_b_own.shape, f32),
            pltpu.SMEM(spread_a.shape, f32), pltpu.SMEM(spread_b.shape, f32),
            pltpu.VMEM((devices, rows_y, deep, LANES), f32),
            pltpu.VMEM((2, rows_y, full_z, LANES), f32),
            pltpu.VMEM((2, wide, tall, full_z), f32),
            pltpu.VMEM((2, halves, wide // 2, BAND, full_z), f32),
            volume, volume, volume, volume,
            pltpu.VMEM((4, wide + 2 * radius, full_y, full_z), f32),
            pltpu.VMEM((2, rows_y, full_z, LANES), f32),
            pltpu.VMEM((devices, rows_y, deep, LANES), f32),
            pltpu.VMEM((4, 2 * full_z, 2 * full_z), bf16), pltpu.VMEM((4, 2 * LANES, 2 * LANES), bf16),
            dma((4,)), dma((halves, devices)), dma((halves, devices)), dma((2, 2, halves)), dma((2, 2, halves)), dma((2, halves)), dma((2, halves)),
            dma((4, bands, 2)), dma((4, bands, 2)), dma((halves, devices)), dma((halves, devices)),
        ],
        compiler_params=pltpu.CompilerParams(
            collective_id=0, has_side_effects=True, vmem_limit_bytes=48 * 1024 * 1024
        ),
    )(*(pltpu.with_memory_space_constraint(x, pltpu.HBM) for x in (view_a, view_b_own, spread_a, spread_b)))
    return jnp.transpose(turned, (1, 0, 2))


def fits_slabs(mesh, view_a, view_b_own, spread_a):
    groups, sides = mesh.shape["gz"], mesh.shape["gy"]
    deep = view_a[0] // (mesh.shape["blocks"] * groups)
    tall, wide = view_a[1] // sides, view_a[2] // (2 * groups)
    return (
        mesh.shape["blocks"] == 2 and groups % 2 == 0 and sides == 2 and wide * QUARTERS == LANES and view_b_own[2] == LANES and 4 * view_a[1] == LANES
        and tall % (8 * sides) == 0 and deep % 8 == 0 and spread_a[1] % 2 == 1 and spread_a[1] // 2 <= wide // 2
    )


def solution(mesh):
    in_specs = (P(("blocks", "gz"), "gy", None), P(("blocks", "gz"), "gy", None), P(), P())
    out_specs = P(("blocks", "gz"), "gy", None)

    def run(view_a, view_b_own, spread_a, spread_b):
        plan = slab_shards if fits_slabs(mesh, view_a.shape, view_b_own.shape, spread_a.shape) else shards
        split_plan = jax.shard_map(plan, mesh=mesh, in_specs=in_specs, out_specs=out_specs, check_vma=False)
        return split_plan(view_a, view_b_own, spread_a, spread_b)

    return run
```

```python
import functools

import jax
import jax.numpy as jnp
from jax import lax
from jax.experimental import pallas as pl
from jax.experimental.pallas import tpu as pltpu
from jax.sharding import PartitionSpec as P

LANES = 128
QUARTERS = 4
BAND = 8


def padded(cells, sides, width):
    for axis, dim in sides:
        count = lax.axis_size(axis)
        ends = count - 1
        head = lax.slice_in_dim(cells, 0, width, axis=dim)
        tail = lax.slice_in_dim(cells, cells.shape[dim] - width, cells.shape[dim], axis=dim)
        cells = jnp.concatenate(
            [
                lax.ppermute(tail, axis, [(i, (i + 1) % count) for i in range(ends)]),
                cells,
                lax.ppermute(head, axis, [((i + 1) % count, i) for i in range(ends)]),
            ],
            axis=dim,
        )
    return cells


def band_table(weights, count_in, count_out, offset):
    source = jnp.arange(count_in, dtype=jnp.int32)[:, None]
    target = jnp.arange(count_out, dtype=jnp.int32)[None, :]
    spread = source - target + offset
    table = jnp.zeros((count_in, count_out), jnp.float32)
    for place in range(weights.shape[0]):
        table = table + jnp.where(spread == place, weights[place], jnp.float32(0.0))
    return table


def blur(volume, kernels):
    count_z, count_y, count_x = volume.shape
    radius = (kernels.shape[1] - 1) // 2
    table_x = band_table(kernels[2], count_x, count_x, radius)
    along_x = jnp.einsum("zyx,xw->zyw", volume, table_x, precision=lax.Precision.HIGHEST)
    table_y = band_table(kernels[1], count_y + 2 * radius, count_y, 0)
    widened = padded(along_x, (("gy", 1),), radius)
    narrow_y = jnp.einsum("zyx,yw->zwx", widened, table_y, precision=lax.Precision.HIGHEST)
    along_y = padded(narrow_y, (("gz", 0),), radius)
    table_z = band_table(kernels[0], count_z + 2 * radius, count_z, 0)
    return jnp.einsum("zyx,zw->wyx", along_y, table_z, precision=lax.Precision.HIGHEST)


def shards(view_a, view_b_own, spread_a, spread_b):
    arrived = lax.all_to_all(view_b_own, "gz", split_axis=2, concat_axis=0, tiled=True)
    view_b = jnp.transpose(arrived, (2, 1, 0))[:, :, ::-1]
    blur_a = spread_a / jnp.sum(spread_a, axis=1, keepdims=True)
    blur_b = spread_b / jnp.sum(spread_b, axis=1, keepdims=True)
    estimate = 0.5 * (view_a + view_b)
    for measured, kernels in ((view_a, blur_a), (view_b, blur_b)):
        quotient = measured / blur(estimate, kernels)
        estimate = estimate * blur(quotient, kernels[:, ::-1])
    return estimate


def block_transpose(parts, width):
    lane = lax.broadcasted_iota(jnp.int32, parts[0].shape, 1)
    for step in (2, 1):
        shift = step * width
        low = lax.rem(lane // shift, 2) == 0
        out = list(parts)
        for first in range(QUARTERS):
            if first & step:
                continue
            second = first + step
            out[first] = jnp.where(low, parts[first], pltpu.roll(parts[second], shift, 1))
            out[second] = jnp.where(low, pltpu.roll(parts[first], LANES - shift, 1), parts[second])
        parts = out
    return parts


def split(values):
    high = values.astype(jnp.bfloat16)
    return high, (values - high.astype(jnp.float32)).astype(jnp.bfloat16)


def dot(a, b):
    return jnp.dot(a, b, preferred_element_type=jnp.float32)


def deconvolve(
    va_hbm, vb_hbm, sa_hbm, sb_hbm, out_ref,
    va_ref, vb_ref, sa_ref, sb_ref,
    send_a, recv_a, recv_b, relay, view_a, view_b, estimate, blurred, wide_x,
    send_e, recv_e, table_z, table_y,
    in_sem, a_send_sem, a_recv_sem, b_send_sem, b_recv_sem, r_send_sem, r_recv_sem, h_send_sem, h_recv_sem, e_send_sem, e_recv_sem,
):
    f32 = jnp.float32
    groups = lax.axis_size("gz")
    devices = 2 * groups
    block = lax.axis_index("blocks")
    gz, gy = lax.axis_index("gz"), lax.axis_index("gy")
    me = 2 * gz + gy
    deep, tall, long_x = va_ref.shape
    wide, full_y, full_z = view_a.shape
    taps = sa_ref.shape[1]
    radius = (taps - 1) // 2
    rows_y = tall // QUARTERS
    bands = full_y // BAND
    side_bands = tall // BAND
    lines = BAND // QUARTERS
    order = [side * side_bands + half for half in range(side_bands) for side in range(2)]
    spreads = (sa_ref, sb_ref)
    mirror = gz + 1 - 2 * lax.rem(gz, 2)
    crossed = lax.rem(gz // 2 + block, 2) == 1
    direct_x = wide // 2

    def snake(group):
        return jnp.where(lax.rem(group // 2 + block, 2) == 1, group + 1 - 2 * lax.rem(group, 2), group)

    def slab_of(device):
        return 2 * (groups - 1 - snake(device // 2)) + lax.rem(device, 2)

    def at(device):
        return (block, device // 2, lax.rem(device, 2))

    def device_of(place):
        return (block, snake(groups - 1 - place // 2), lax.rem(place, 2))

    slab = slab_of(me)

    def remote(src, dst, send_sem, recv_sem, device):
        return pltpu.make_async_remote_copy(
            src_ref=src, dst_ref=dst, send_sem=send_sem, recv_sem=recv_sem,
            device_id=device, device_id_type=pl.DeviceIdType.MESH,
        )

    barrier = pltpu.get_barrier_semaphore()
    for hop in range(1, devices):
        pl.semaphore_signal(
            barrier, inc=1, device_id=at(lax.rem(me + hop, devices)), device_id_type=pl.DeviceIdType.MESH
        )

    for group, core in ((gz, gy), (mirror, 0), (mirror, 1)):
        pl.semaphore_signal(
            barrier, inc=1, device_id=(1 - block, group, core), device_id_type=pl.DeviceIdType.MESH
        )

    loads = [
        pltpu.make_async_copy(src, dst, in_sem.at[index])
        for index, (src, dst) in enumerate(
            ((va_hbm, va_ref), (vb_hbm, vb_ref), (sa_hbm, sa_ref), (sb_hbm, sb_ref))
        )
    ]
    for load in loads:
        load.start()
    loads[0].wait()
    for y in range(rows_y):
        for column in range(long_x // LANES):
            pieces = [
                va_ref[:, QUARTERS * y + q, column * LANES:(column + 1) * LANES] for q in range(QUARTERS)
            ]
            for k, piece in enumerate(block_transpose(pieces, wide)):
                send_a[QUARTERS * column + k, y] = piece

    loads[1].wait()
    pl.semaphore_wait(barrier, devices + 2)

    half = remote(
        vb_ref.at[pl.ds(wide * gy, wide)], recv_b.at[gy], b_send_sem.at[0, 0, 0], b_recv_sem.at[gy, 0, 0], (block, gz, 1 - gy)
    )

    def direct(core, part):
        ys = pl.ds(BAND * part, BAND)
        return remote(
            vb_ref.at[pl.ds(wide * (1 - core), direct_x), ys], recv_b.at[gy, pl.ds(0, direct_x), ys],
            b_send_sem.at[core, 0, part], b_recv_sem.at[gy, 0, part], (block, mirror, core),
        )

    def detour(core, part):
        ys = pl.ds(BAND * part, BAND)
        return remote(
            vb_ref.at[pl.ds(wide * (1 - core) + direct_x, wide - direct_x), ys], relay.at[core, part],
            b_send_sem.at[core, 1, part], r_recv_sem.at[core, part], (1 - block, gz, gy),
        )

    def onward(core, part):
        ys = pl.ds(BAND * part, BAND)
        return remote(
            relay.at[core, part], recv_b.at[gy, pl.ds(direct_x, wide - direct_x), ys],
            r_send_sem.at[core, part], b_recv_sem.at[gy, 1, part], (1 - block, mirror, core),
        )

    @pl.when(crossed)
    def _():
        for part in range(side_bands):
            for core in range(2):
                detour(core, part).start()

    pl.when(jnp.logical_not(crossed))(half.start)
    own_z = pl.ds(pl.multiple_of(gz * deep, 8), deep)

    def copy_a(part, hop):
        target = lax.rem(me + hop, devices)
        rows = pl.ds(lines * part, lines)
        return remote(
            send_a.at[slab_of(target), rows], recv_a.at[gy, rows, own_z],
            a_send_sem.at[part, hop], a_recv_sem.at[part, hop], at(target),
        )

    for part in range(side_bands):
        for hop in range(1, devices):
            copy_a(part, hop).start()

        @pl.when(crossed)
        def _():
            for core in range(2):
                direct(core, part).start()

    recv_a[gy, :, own_z] = send_a[slab]

    loads[2].wait()
    loads[3].wait()
    row = lax.broadcasted_iota(jnp.int32, (full_z, LANES), 0)
    col = lax.broadcasted_iota(jnp.int32, (full_z, LANES), 1)
    for which, spread in enumerate(spreads):
        total = f32(1.0)
        for axis in range(3):
            line = spread[axis, 0]
            for tap in range(1, taps):
                line = line + spread[axis, tap]
            total = total * line
        for flipped in range(2):
            index = 2 * which + flipped
            sign = -1 if flipped else 1
            offset = sign * (row - col) + radius
            table = jnp.zeros((full_z, LANES), f32)
            for tap in range(taps):
                table = jnp.where(offset == tap, spread[0, tap], table)
            table = table / jnp.full((full_z, LANES), total, f32)
            high, low = split(table)
            blank = jnp.zeros((full_z, LANES), jnp.bfloat16)
            table_z[index] = jnp.concatenate(
                [jnp.concatenate([high, low], axis=1), jnp.concatenate([high, blank], axis=1)], axis=0
            )
            offset = jnp.where(row // full_y == col // full_y, sign * (col - row) + radius, -1)
            table = jnp.zeros((LANES, LANES), f32)
            for tap in range(taps):
                table = jnp.where(offset == tap, spread[1, tap], table)
            high, low = split(table)
            blank = jnp.zeros((LANES, LANES), jnp.bfloat16)
            table_y[index] = jnp.concatenate(
                [jnp.concatenate([high, high], axis=1), jnp.concatenate([low, blank], axis=1)], axis=0
            )

    mine = pl.multiple_of(gy * tall, BAND)

    @pl.when(jnp.logical_not(crossed))
    def _():
        for part in range(side_bands):
            for core in range(2):
                detour(core, part).wait_recv()
                onward(core, part).start()
        for x in range(wide):
            view_b[x, pl.ds(mine, tall)] = vb_ref[2 * wide - 1 - wide * gy - x]
        remote(
            vb_ref.at[pl.ds(0, wide)], recv_b.at[0], b_send_sem.at[0, 0, 0], b_recv_sem.at[1 - gy, 0, 0],
            (block, gz, 1 - gy),
        ).wait_recv()
        other = pl.multiple_of((1 - gy) * tall, BAND)
        for x in range(wide):
            view_b[x, pl.ds(other, tall)] = recv_b[1 - gy, wide - 1 - x]

    def crossed_view(part):
        for core in range(2):
            ys = pl.ds(BAND * part, BAND)
            remote(
                vb_ref.at[pl.ds(0, direct_x), ys], recv_b.at[core, pl.ds(0, direct_x), ys],
                b_send_sem.at[0, 0, part], b_recv_sem.at[core, 0, part], (block, mirror, core),
            ).wait_recv()
            remote(
                relay.at[0, part], recv_b.at[core, pl.ds(direct_x, wide - direct_x), ys],
                r_send_sem.at[0, part], b_recv_sem.at[core, 1, part], (1 - block, mirror, core),
            ).wait_recv()
            for x in range(wide):
                view_b[x, core * tall + BAND * part:core * tall + BAND * (part + 1)] = recv_b[core, wide - 1 - x, ys]

    outer = jnp.where(gy == 0, slab > 0, slab < devices - 1)
    neighbour = device_of(jnp.clip(slab + 2 * gy - 1, 0, devices - 1))

    @pl.when(jnp.logical_not(outer))
    def _():
        for turn in range(4):
            wide_x[turn, pl.ds((radius + wide) * gy, radius)] = jnp.zeros((radius, full_y, full_z), f32)

    def halo(turn, band, inner):
        ys = pl.ds(band * BAND, BAND) if isinstance(band, int) else pl.ds(pl.multiple_of(band * BAND, BAND), BAND)
        source = radius + (wide - radius) * ((1 - gy) if inner else gy)
        target = (radius + wide) * (gy if inner else (1 - gy))
        return remote(
            wide_x.at[turn, pl.ds(source, radius), ys], wide_x.at[turn, pl.ds(target, radius), ys],
            h_send_sem.at[turn, band, inner], h_recv_sem.at[turn, band, inner],
            (block, gz, 1 - gy) if inner else neighbour,
        )

    def send_outer(turn, band):
        pl.when(outer)(halo(turn, band, 0).start)

    def send_inner(turn, band):
        halo(turn, band, 1).start()

    def await_halos(turn, band):
        halo(turn, band, 1).wait_recv()
        pl.when(outer)(halo(turn, band, 0).wait_recv)

    def x_taps(turn, which, flipped, band, edges, finish):
        ys = pl.ds(band * BAND, BAND) if isinstance(band, int) else pl.ds(pl.multiple_of(band * BAND, BAND), BAND)
        spread = spreads[which]
        weights = [spread[2, taps - 1 - tap if flipped else tap] for tap in range(taps)]
        for x in range(wide):
            total = blurred[x, ys] if edges else None
            for tap in range(taps):
                place = x + tap
                if (radius <= place < radius + wide) != edges:
                    term = weights[tap] * wide_x[turn, place, ys]
                    total = term if total is None else total + term
            finish(x, ys, total)

    def keep(x, ys, total):
        blurred[x, ys] = total

    for part in range(side_bands):
        pl.when(crossed)(functools.partial(crossed_view, part))
        for side in range(2):
            for group in range(groups):
                hop = lax.rem(me - 2 * group - side + devices, devices)
                pl.when(hop != 0)(copy_a(part, hop).wait_recv)
            for y in range(lines * part, lines * (part + 1)):
                turned = recv_a[side, y].T
                for q in range(QUARTERS):
                    view_a[:, side * tall + QUARTERS * y + q, :] = turned[q * wide:(q + 1) * wide]
            band = side * side_bands + part
            ys = pl.ds(band * BAND, BAND)
            start = 0.5 * (view_a[:, ys] + view_b[:, ys])
            estimate[:, ys] = start
            wide_x[0, pl.ds(radius, wide), ys] = start
            send_outer(0, band)
            send_inner(0, band)

    planes = LANES // full_y
    chunks = wide // planes // 2

    def along_zy(values, index):
        high, low = split(values.reshape(chunks * LANES, full_z))
        both = dot(jnp.concatenate([high, low], axis=1), table_z[index])
        high, low = split(both[:, :LANES] + both[:, LANES:])
        outs = []
        for chunk in range(0, chunks, 2):
            first = slice(chunk * LANES, (chunk + 1) * LANES)
            second = slice((chunk + 1) * LANES, (chunk + 2) * LANES)
            stacked = jnp.concatenate(
                [
                    jnp.concatenate([high[first], high[second]], axis=1),
                    jnp.concatenate([low[first], low[second]], axis=1),
                ],
                axis=0,
            )
            both = dot(table_y[index], stacked)
            both = both[:LANES] + both[LANES:]
            outs += [both[:, :LANES], both[:, LANES:]]
        return jnp.concatenate(outs, axis=0).reshape(wide // 2, full_y, full_z)

    def middle(turn, which, view):
        for step in range(2):
            first = (wide // 2) * (gy if step == 0 else 1 - gy)
            span = pl.ds(first, wide // 2)
            quotient = view[span] / along_zy(blurred[span], 2 * which)
            wide_x[turn, pl.ds(radius + first, wide // 2)] = along_zy(quotient, 2 * which + 1)
            for band in order:
                (send_inner if step else send_outer)(turn, band)

    def looped(body):
        def step(index, carry):
            body(lax.rem(index, 2) * side_bands + index // 2)
            return carry

        lax.fori_loop(0, bands, step, 0)

    looped(lambda band: x_taps(0, 0, 0, band, False, keep))

    def first_edges(band):
        await_halos(0, band)
        x_taps(0, 0, 0, band, True, keep)

    looped(first_edges)
    middle(1, 0, view_a)
    looped(lambda band: x_taps(1, 0, 1, band, False, keep))

    def update(x, ys, total):
        value = estimate[x, ys] * total
        estimate[x, ys] = value
        wide_x[2, radius + x, ys] = value

    def second_edges(band):
        await_halos(1, band)
        x_taps(1, 0, 1, band, True, update)
        send_outer(2, band)
        send_inner(2, band)
        x_taps(2, 1, 0, band, False, keep)

    looped(second_edges)

    def third_edges(band):
        await_halos(2, band)
        x_taps(2, 1, 0, band, True, keep)

    looped(third_edges)
    middle(3, 1, view_b)
    looped(lambda band: x_taps(3, 1, 1, band, False, keep))

    def last(x, ys, total):
        estimate[x, ys] = estimate[x, ys] * total

    def copy_e(side, part, step):
        target = 2 * step + side
        hop = lax.rem(target - me + devices, devices)
        rows = pl.ds(lines * part, lines)
        return remote(
            send_e.at[side, rows, pl.ds(pl.multiple_of(target // 2 * deep, 8), deep)], recv_e.at[slab, rows],
            e_send_sem.at[part, hop], e_recv_sem.at[part, hop], at(target),
        )

    far = gz >= groups // 2
    for band in order:
        side, part = band // side_bands, band % side_bands
        await_halos(3, band)
        x_taps(3, 1, 1, band, True, last)
        for y in range(lines * part, lines * (part + 1)):
            strips = [estimate[:, side * tall + QUARTERS * y + q, :] for q in range(QUARTERS)]
            send_e[side, y] = jnp.concatenate(strips, axis=0).T
        for step in range(groups):
            now = jnp.logical_not(far) if 2 <= step < groups // 2 else True
            pl.when(jnp.logical_and(me != 2 * step + side, now))(copy_e(side, part, step).start)

    @pl.when(far)
    def _():
        for band in order:
            for step in range(2, groups // 2):
                copy_e(band // side_bands, band % side_bands, step).start()

    recv_e[slab] = send_e[gy, :, own_z]
    columns = long_x // LANES

    def arrived_e(part, place):
        source = 2 * snake(groups - 1 - place // 2) + lax.rem(place, 2)
        hop = lax.rem(me - source + devices, devices)
        pl.when(hop != 0)(
            remote(
                send_e.at[0, pl.ds(0, lines), pl.ds(0, deep)], recv_e.at[place, pl.ds(lines * part, lines)],
                e_send_sem.at[part, hop], e_recv_sem.at[part, hop], at(lax.rem(me + hop, devices)),
            ).wait_recv
        )

    for part in range(side_bands):
        for step in range(columns):
            column = jnp.where(gz < groups // 2, columns - 1 - step, step)
            xs = pl.ds(pl.multiple_of(column * LANES, LANES), LANES)
            for k in range(QUARTERS):
                arrived_e(part, QUARTERS * column + k)
            for y in range(lines * part, lines * (part + 1)):
                pieces = [recv_e[QUARTERS * column + k, y] for k in range(QUARTERS)]
                for q, piece in enumerate(block_transpose(pieces, wide)):
                    out_ref[QUARTERS * y + q, :, xs] = piece

    for part in range(side_bands):
        for hop in range(1, devices):
            copy_a(part, hop).wait_send()
        for side in range(2):
            for step in range(groups):
                pl.when(me != 2 * step + side)(copy_e(side, part, step).wait_send)

    @pl.when(crossed)
    def _():
        for part in range(side_bands):
            for core in range(2):
                detour(core, part).wait_send()
                direct(core, part).wait_send()

    @pl.when(jnp.logical_not(crossed))
    def _():
        half.wait_send()
        for part in range(side_bands):
            for core in range(2):
                onward(core, part).wait_send()

    for turn in range(4):
        for band in range(bands):
            halo(turn, band, 1).wait_send()
            pl.when(outer)(halo(turn, band, 0).wait_send)


def slab_shards(view_a, view_b_own, spread_a, spread_b):
    groups = lax.axis_size("gz")
    deep, tall, long_x = view_a.shape
    devices = 2 * groups
    wide = long_x // devices
    full_y, full_z = 2 * tall, view_b_own.shape[2]
    taps = spread_a.shape[1]
    radius = (taps - 1) // 2
    f32, bf16 = jnp.float32, jnp.bfloat16
    volume = pltpu.VMEM((wide, full_y, full_z), f32)
    rows_y = tall // QUARTERS
    bands, halves = full_y // BAND, tall // BAND
    dma = pltpu.SemaphoreType.DMA
    turned = pl.pallas_call(
        deconvolve,
        out_shape=jax.ShapeDtypeStruct((tall, deep, long_x), f32),
        in_specs=[pl.BlockSpec(memory_space=pl.ANY)] * 4,
        out_specs=pl.BlockSpec(memory_space=pltpu.VMEM),
        scratch_shapes=[
            pltpu.VMEM(view_a.shape, f32), pltpu.VMEM(view_b_own.shape, f32),
            pltpu.SMEM(spread_a.shape, f32), pltpu.SMEM(spread_b.shape, f32),
            pltpu.VMEM((devices, rows_y, deep, LANES), f32),
            pltpu.VMEM((2, rows_y, full_z, LANES), f32),
            pltpu.VMEM((2, wide, tall, full_z), f32),
            pltpu.VMEM((2, halves, wide // 2, BAND, full_z), f32),
            volume, volume, volume, volume,
            pltpu.VMEM((4, wide + 2 * radius, full_y, full_z), f32),
            pltpu.VMEM((2, rows_y, full_z, LANES), f32),
            pltpu.VMEM((devices, rows_y, deep, LANES), f32),
            pltpu.VMEM((4, 2 * full_z, 2 * full_z), bf16), pltpu.VMEM((4, 2 * LANES, 2 * LANES), bf16),
            dma((4,)), dma((halves, devices)), dma((halves, devices)), dma((2, 2, halves)), dma((2, 2, halves)), dma((2, halves)), dma((2, halves)),
            dma((4, bands, 2)), dma((4, bands, 2)), dma((halves, devices)), dma((halves, devices)),
        ],
        compiler_params=pltpu.CompilerParams(
            collective_id=0, has_side_effects=True, vmem_limit_bytes=48 * 1024 * 1024
        ),
    )(*(pltpu.with_memory_space_constraint(x, pltpu.HBM) for x in (view_a, view_b_own, spread_a, spread_b)))
    return jnp.transpose(turned, (1, 0, 2))


def fits_slabs(mesh, view_a, view_b_own, spread_a):
    groups, sides = mesh.shape["gz"], mesh.shape["gy"]
    deep = view_a[0] // (mesh.shape["blocks"] * groups)
    tall, wide = view_a[1] // sides, view_a[2] // (2 * groups)
    return (
        mesh.shape["blocks"] == 2 and groups % 2 == 0 and sides == 2 and wide * QUARTERS == LANES and view_b_own[2] == LANES and 4 * view_a[1] == LANES
        and tall % (8 * sides) == 0 and deep % 8 == 0 and spread_a[1] % 2 == 1 and spread_a[1] // 2 <= wide // 2
    )


def solution(mesh):
    in_specs = (P(("blocks", "gz"), "gy", None), P(("blocks", "gz"), "gy", None), P(), P())
    out_specs = P(("blocks", "gz"), "gy", None)

    def run(view_a, view_b_own, spread_a, spread_b):
        plan = slab_shards if fits_slabs(mesh, view_a.shape, view_b_own.shape, spread_a.shape) else shards
        split_plan = jax.shard_map(plan, mesh=mesh, in_specs=in_specs, out_specs=out_specs, check_vma=False)
        return split_plan(view_a, view_b_own, spread_a, spread_b)

    return run
```

```python
import functools

import jax
import jax.numpy as jnp
from jax import lax
from jax.experimental import pallas as pl
from jax.experimental.pallas import tpu as pltpu
from jax.sharding import PartitionSpec as P

LANES = 128
QUARTERS = 4
BAND = 8


def padded(cells, sides, width):
    for axis, dim in sides:
        count = lax.axis_size(axis)
        ends = count - 1
        head = lax.slice_in_dim(cells, 0, width, axis=dim)
        tail = lax.slice_in_dim(cells, cells.shape[dim] - width, cells.shape[dim], axis=dim)
        cells = jnp.concatenate(
            [
                lax.ppermute(tail, axis, [(i, (i + 1) % count) for i in range(ends)]),
                cells,
                lax.ppermute(head, axis, [((i + 1) % count, i) for i in range(ends)]),
            ],
            axis=dim,
        )
    return cells


def band_table(weights, count_in, count_out, offset):
    source = jnp.arange(count_in, dtype=jnp.int32)[:, None]
    target = jnp.arange(count_out, dtype=jnp.int32)[None, :]
    spread = source - target + offset
    table = jnp.zeros((count_in, count_out), jnp.float32)
    for place in range(weights.shape[0]):
        table = table + jnp.where(spread == place, weights[place], jnp.float32(0.0))
    return table


def blur(volume, kernels):
    count_z, count_y, count_x = volume.shape
    radius = (kernels.shape[1] - 1) // 2
    table_x = band_table(kernels[2], count_x, count_x, radius)
    along_x = jnp.einsum("zyx,xw->zyw", volume, table_x, precision=lax.Precision.HIGHEST)
    table_y = band_table(kernels[1], count_y + 2 * radius, count_y, 0)
    widened = padded(along_x, (("gy", 1),), radius)
    narrow_y = jnp.einsum("zyx,yw->zwx", widened, table_y, precision=lax.Precision.HIGHEST)
    along_y = padded(narrow_y, (("gz", 0),), radius)
    table_z = band_table(kernels[0], count_z + 2 * radius, count_z, 0)
    return jnp.einsum("zyx,zw->wyx", along_y, table_z, precision=lax.Precision.HIGHEST)


def shards(view_a, view_b_own, spread_a, spread_b):
    arrived = lax.all_to_all(view_b_own, "gz", split_axis=2, concat_axis=0, tiled=True)
    view_b = jnp.transpose(arrived, (2, 1, 0))[:, :, ::-1]
    blur_a = spread_a / jnp.sum(spread_a, axis=1, keepdims=True)
    blur_b = spread_b / jnp.sum(spread_b, axis=1, keepdims=True)
    estimate = 0.5 * (view_a + view_b)
    for measured, kernels in ((view_a, blur_a), (view_b, blur_b)):
        quotient = measured / blur(estimate, kernels)
        estimate = estimate * blur(quotient, kernels[:, ::-1])
    return estimate


def block_transpose(parts, width):
    lane = lax.broadcasted_iota(jnp.int32, parts[0].shape, 1)
    for step in (2, 1):
        shift = step * width
        low = lax.rem(lane // shift, 2) == 0
        out = list(parts)
        for first in range(QUARTERS):
            if first & step:
                continue
            second = first + step
            out[first] = jnp.where(low, parts[first], pltpu.roll(parts[second], shift, 1))
            out[second] = jnp.where(low, pltpu.roll(parts[first], LANES - shift, 1), parts[second])
        parts = out
    return parts


def split(values):
    high = values.astype(jnp.bfloat16)
    return high, (values - high.astype(jnp.float32)).astype(jnp.bfloat16)


def dot(a, b):
    return jnp.dot(a, b, preferred_element_type=jnp.float32)


def deconvolve(
    va_hbm, vb_hbm, sa_hbm, sb_hbm, out_ref,
    va_ref, vb_ref, sa_ref, sb_ref,
    send_a, recv_a, recv_b, relay, view_a, view_b, estimate, blurred, wide_x,
    send_e, recv_e, table_z, table_y,
    in_sem, a_send_sem, a_recv_sem, b_send_sem, b_recv_sem, r_send_sem, r_recv_sem, h_send_sem, h_recv_sem, e_send_sem, e_recv_sem,
):
    f32 = jnp.float32
    groups = lax.axis_size("gz")
    devices = 2 * groups
    block = lax.axis_index("blocks")
    gz, gy = lax.axis_index("gz"), lax.axis_index("gy")
    me = 2 * gz + gy
    deep, tall, long_x = va_ref.shape
    wide, full_y, full_z = view_a.shape
    taps = sa_ref.shape[1]
    radius = (taps - 1) // 2
    rows_y = tall // QUARTERS
    bands = full_y // BAND
    side_bands = tall // BAND
    lines = BAND // QUARTERS
    order = [side * side_bands + half for half in range(side_bands) for side in range(2)]
    spreads = (sa_ref, sb_ref)
    mirror = gz + 1 - 2 * lax.rem(gz, 2)
    crossed = lax.rem(gz // 2 + block, 2) == 1
    direct_x = wide // 2

    def snake(group):
        return jnp.where(lax.rem(group // 2 + block, 2) == 1, group + 1 - 2 * lax.rem(group, 2), group)

    def slab_of(device):
        return 2 * (groups - 1 - snake(device // 2)) + lax.rem(device, 2)

    def at(device):
        return (block, device // 2, lax.rem(device, 2))

    def device_of(place):
        return (block, snake(groups - 1 - place // 2), lax.rem(place, 2))

    slab = slab_of(me)

    def remote(src, dst, send_sem, recv_sem, device):
        return pltpu.make_async_remote_copy(
            src_ref=src, dst_ref=dst, send_sem=send_sem, recv_sem=recv_sem,
            device_id=device, device_id_type=pl.DeviceIdType.MESH,
        )

    barrier = pltpu.get_barrier_semaphore()
    for hop in range(1, devices):
        pl.semaphore_signal(
            barrier, inc=1, device_id=at(lax.rem(me + hop, devices)), device_id_type=pl.DeviceIdType.MESH
        )

    for group, core in ((gz, gy), (mirror, 0), (mirror, 1)):
        pl.semaphore_signal(
            barrier, inc=1, device_id=(1 - block, group, core), device_id_type=pl.DeviceIdType.MESH
        )

    loads = [
        pltpu.make_async_copy(src, dst, in_sem.at[index])
        for index, (src, dst) in enumerate(
            ((va_hbm, va_ref), (vb_hbm, vb_ref), (sa_hbm, sa_ref), (sb_hbm, sb_ref))
        )
    ]
    for load in loads:
        load.start()
    loads[0].wait()
    for y in range(rows_y):
        for column in range(long_x // LANES):
            pieces = [
                va_ref[:, QUARTERS * y + q, column * LANES:(column + 1) * LANES] for q in range(QUARTERS)
            ]
            for k, piece in enumerate(block_transpose(pieces, wide)):
                send_a[QUARTERS * column + k, y] = piece

    loads[1].wait()
    pl.semaphore_wait(barrier, devices + 2)

    half = remote(
        vb_ref.at[pl.ds(wide * gy, wide)], recv_b.at[gy], b_send_sem.at[0, 0, 0], b_recv_sem.at[gy, 0, 0], (block, gz, 1 - gy)
    )

    def direct(core, part):
        ys = pl.ds(BAND * part, BAND)
        return remote(
            vb_ref.at[pl.ds(wide * (1 - core), direct_x), ys], recv_b.at[gy, pl.ds(0, direct_x), ys],
            b_send_sem.at[core, 0, part], b_recv_sem.at[gy, 0, part], (block, mirror, core),
        )

    def detour(core, part):
        ys = pl.ds(BAND * part, BAND)
        return remote(
            vb_ref.at[pl.ds(wide * (1 - core) + direct_x, wide - direct_x), ys], relay.at[core, part],
            b_send_sem.at[core, 1, part], r_recv_sem.at[core, part], (1 - block, gz, gy),
        )

    def onward(core, part):
        ys = pl.ds(BAND * part, BAND)
        return remote(
            relay.at[core, part], recv_b.at[gy, pl.ds(direct_x, wide - direct_x), ys],
            r_send_sem.at[core, part], b_recv_sem.at[gy, 1, part], (1 - block, mirror, core),
        )

    @pl.when(crossed)
    def _():
        for part in range(side_bands):
            for core in range(2):
                detour(core, part).start()

    pl.when(jnp.logical_not(crossed))(half.start)
    own_z = pl.ds(pl.multiple_of(gz * deep, 8), deep)

    def copy_a(part, hop):
        target = lax.rem(me + hop, devices)
        rows = pl.ds(lines * part, lines)
        return remote(
            send_a.at[slab_of(target), rows], recv_a.at[gy, rows, own_z],
            a_send_sem.at[part, hop], a_recv_sem.at[part, hop], at(target),
        )

    for part in range(side_bands):
        for hop in range(1, devices):
            copy_a(part, hop).start()

        @pl.when(crossed)
        def _():
            for core in range(2):
                direct(core, part).start()

    recv_a[gy, :, own_z] = send_a[slab]

    loads[2].wait()
    loads[3].wait()
    row = lax.broadcasted_iota(jnp.int32, (full_z, LANES), 0)
    col = lax.broadcasted_iota(jnp.int32, (full_z, LANES), 1)
    for which, spread in enumerate(spreads):
        total = f32(1.0)
        for axis in range(3):
            line = spread[axis, 0]
            for tap in range(1, taps):
                line = line + spread[axis, tap]
            total = total * line
        for flipped in range(2):
            index = 2 * which + flipped
            sign = -1 if flipped else 1
            offset = sign * (row - col) + radius
            table = jnp.zeros((full_z, LANES), f32)
            for tap in range(taps):
                table = jnp.where(offset == tap, spread[0, tap], table)
            table = table / jnp.full((full_z, LANES), total, f32)
            high, low = split(table)
            blank = jnp.zeros((full_z, LANES), jnp.bfloat16)
            table_z[index] = jnp.concatenate(
                [jnp.concatenate([high, low], axis=1), jnp.concatenate([high, blank], axis=1)], axis=0
            )
            offset = jnp.where(row // full_y == col // full_y, sign * (col - row) + radius, -1)
            table = jnp.zeros((LANES, LANES), f32)
            for tap in range(taps):
                table = jnp.where(offset == tap, spread[1, tap], table)
            high, low = split(table)
            blank = jnp.zeros((LANES, LANES), jnp.bfloat16)
            table_y[index] = jnp.concatenate(
                [jnp.concatenate([high, high], axis=1), jnp.concatenate([low, blank], axis=1)], axis=0
            )

    mine = pl.multiple_of(gy * tall, BAND)

    @pl.when(jnp.logical_not(crossed))
    def _():
        for part in range(side_bands):
            for core in range(2):
                detour(core, part).wait_recv()
                onward(core, part).start()
        for x in range(wide):
            view_b[x, pl.ds(mine, tall)] = vb_ref[2 * wide - 1 - wide * gy - x]
        remote(
            vb_ref.at[pl.ds(0, wide)], recv_b.at[0], b_send_sem.at[0, 0, 0], b_recv_sem.at[1 - gy, 0, 0],
            (block, gz, 1 - gy),
        ).wait_recv()
        other = pl.multiple_of((1 - gy) * tall, BAND)
        for x in range(wide):
            view_b[x, pl.ds(other, tall)] = recv_b[1 - gy, wide - 1 - x]

    def crossed_view(part):
        for core in range(2):
            ys = pl.ds(BAND * part, BAND)
            remote(
                vb_ref.at[pl.ds(0, direct_x), ys], recv_b.at[core, pl.ds(0, direct_x), ys],
                b_send_sem.at[0, 0, part], b_recv_sem.at[core, 0, part], (block, mirror, core),
            ).wait_recv()
            remote(
                relay.at[0, part], recv_b.at[core, pl.ds(direct_x, wide - direct_x), ys],
                r_send_sem.at[0, part], b_recv_sem.at[core, 1, part], (1 - block, mirror, core),
            ).wait_recv()
            for x in range(wide):
                view_b[x, core * tall + BAND * part:core * tall + BAND * (part + 1)] = recv_b[core, wide - 1 - x, ys]

    outer = jnp.where(gy == 0, slab > 0, slab < devices - 1)
    neighbour = device_of(jnp.clip(slab + 2 * gy - 1, 0, devices - 1))

    @pl.when(jnp.logical_not(outer))
    def _():
        for turn in range(4):
            wide_x[turn, pl.ds((radius + wide) * gy, radius)] = jnp.zeros((radius, full_y, full_z), f32)

    def halo(turn, band, inner):
        ys = pl.ds(band * BAND, BAND) if isinstance(band, int) else pl.ds(pl.multiple_of(band * BAND, BAND), BAND)
        source = radius + (wide - radius) * ((1 - gy) if inner else gy)
        target = (radius + wide) * (gy if inner else (1 - gy))
        return remote(
            wide_x.at[turn, pl.ds(source, radius), ys], wide_x.at[turn, pl.ds(target, radius), ys],
            h_send_sem.at[turn, band, inner], h_recv_sem.at[turn, band, inner],
            (block, gz, 1 - gy) if inner else neighbour,
        )

    def send_outer(turn, band):
        pl.when(outer)(halo(turn, band, 0).start)

    def send_inner(turn, band):
        halo(turn, band, 1).start()

    def await_halos(turn, band):
        halo(turn, band, 1).wait_recv()
        pl.when(outer)(halo(turn, band, 0).wait_recv)

    def x_taps(turn, which, flipped, band, edges, finish):
        ys = pl.ds(band * BAND, BAND) if isinstance(band, int) else pl.ds(pl.multiple_of(band * BAND, BAND), BAND)
        spread = spreads[which]
        weights = [spread[2, taps - 1 - tap if flipped else tap] for tap in range(taps)]
        for x in range(wide):
            total = blurred[x, ys] if edges else None
            for tap in range(taps):
                place = x + tap
                if (radius <= place < radius + wide) != edges:
                    term = weights[tap] * wide_x[turn, place, ys]
                    total = term if total is None else total + term
            finish(x, ys, total)

    def keep(x, ys, total):
        blurred[x, ys] = total

    for part in range(side_bands):
        pl.when(crossed)(functools.partial(crossed_view, part))
        for side in range(2):
            for group in range(groups):
                hop = lax.rem(me - 2 * group - side + devices, devices)
                pl.when(hop != 0)(copy_a(part, hop).wait_recv)
            for y in range(lines * part, lines * (part + 1)):
                turned = recv_a[side, y].T
                for q in range(QUARTERS):
                    view_a[:, side * tall + QUARTERS * y + q, :] = turned[q * wide:(q + 1) * wide]
            band = side * side_bands + part
            ys = pl.ds(band * BAND, BAND)
            start = 0.5 * (view_a[:, ys] + view_b[:, ys])
            estimate[:, ys] = start
            wide_x[0, pl.ds(radius, wide), ys] = start
            send_outer(0, band)
            send_inner(0, band)

    planes = LANES // full_y
    chunks = wide // planes // 2

    def along_zy(values, index):
        high, low = split(values.reshape(chunks * LANES, full_z))
        both = dot(jnp.concatenate([high, low], axis=1), table_z[index])
        high, low = split(both[:, :LANES] + both[:, LANES:])
        outs = []
        for chunk in range(0, chunks, 2):
            first = slice(chunk * LANES, (chunk + 1) * LANES)
            second = slice((chunk + 1) * LANES, (chunk + 2) * LANES)
            stacked = jnp.concatenate(
                [
                    jnp.concatenate([high[first], high[second]], axis=1),
                    jnp.concatenate([low[first], low[second]], axis=1),
                ],
                axis=0,
            )
            both = dot(table_y[index], stacked)
            both = both[:LANES] + both[LANES:]
            outs += [both[:, :LANES], both[:, LANES:]]
        return jnp.concatenate(outs, axis=0).reshape(wide // 2, full_y, full_z)

    def middle(turn, which, view):
        for step in range(2):
            first = (wide // 2) * (gy if step == 0 else 1 - gy)
            span = pl.ds(first, wide // 2)
            quotient = view[span] / along_zy(blurred[span], 2 * which)
            wide_x[turn, pl.ds(radius + first, wide // 2)] = along_zy(quotient, 2 * which + 1)
            for band in order:
                (send_inner if step else send_outer)(turn, band)

    def looped(body):
        def step(index, carry):
            body(lax.rem(index, 2) * side_bands + index // 2)
            return carry

        lax.fori_loop(0, bands, step, 0)

    looped(lambda band: x_taps(0, 0, 0, band, False, keep))

    def first_edges(band):
        await_halos(0, band)
        x_taps(0, 0, 0, band, True, keep)

    looped(first_edges)
    middle(1, 0, view_a)
    looped(lambda band: x_taps(1, 0, 1, band, False, keep))

    def update(x, ys, total):
        value = estimate[x, ys] * total
        estimate[x, ys] = value
        wide_x[2, radius + x, ys] = value

    def second_edges(band):
        await_halos(1, band)
        x_taps(1, 0, 1, band, True, update)
        send_outer(2, band)
        send_inner(2, band)

    looped(second_edges)

    def third_edges(band):
        x_taps(2, 1, 0, band, False, keep)
        await_halos(2, band)
        x_taps(2, 1, 0, band, True, keep)

    looped(third_edges)
    middle(3, 1, view_b)
    looped(lambda band: x_taps(3, 1, 1, band, False, keep))

    def last(x, ys, total):
        estimate[x, ys] = estimate[x, ys] * total

    def copy_e(side, part, step):
        target = 2 * step + side
        hop = lax.rem(target - me + devices, devices)
        rows = pl.ds(lines * part, lines)
        return remote(
            send_e.at[side, rows, pl.ds(pl.multiple_of(target // 2 * deep, 8), deep)], recv_e.at[slab, rows],
            e_send_sem.at[part, hop], e_recv_sem.at[part, hop], at(target),
        )

    far = gz >= groups // 2
    for band in order:
        side, part = band // side_bands, band % side_bands
        await_halos(3, band)
        x_taps(3, 1, 1, band, True, last)
        for y in range(lines * part, lines * (part + 1)):
            strips = [estimate[:, side * tall + QUARTERS * y + q, :] for q in range(QUARTERS)]
            send_e[side, y] = jnp.concatenate(strips, axis=0).T
        for step in range(groups):
            now = jnp.logical_not(far) if 2 <= step < groups // 2 else True
            pl.when(jnp.logical_and(me != 2 * step + side, now))(copy_e(side, part, step).start)

    @pl.when(far)
    def _():
        for band in order:
            for step in range(2, groups // 2):
                copy_e(band // side_bands, band % side_bands, step).start()

    recv_e[slab] = send_e[gy, :, own_z]
    columns = long_x // LANES

    def arrived_e(part, place):
        source = 2 * snake(groups - 1 - place // 2) + lax.rem(place, 2)
        hop = lax.rem(me - source + devices, devices)
        pl.when(hop != 0)(
            remote(
                send_e.at[0, pl.ds(0, lines), pl.ds(0, deep)], recv_e.at[place, pl.ds(lines * part, lines)],
                e_send_sem.at[part, hop], e_recv_sem.at[part, hop], at(lax.rem(me + hop, devices)),
            ).wait_recv
        )

    for part in range(side_bands):
        for step in range(columns):
            column = jnp.where(gz < groups // 2, columns - 1 - step, step)
            xs = pl.ds(pl.multiple_of(column * LANES, LANES), LANES)
            for k in range(QUARTERS):
                arrived_e(part, QUARTERS * column + k)
            for y in range(lines * part, lines * (part + 1)):
                pieces = [recv_e[QUARTERS * column + k, y] for k in range(QUARTERS)]
                for q, piece in enumerate(block_transpose(pieces, wide)):
                    out_ref[QUARTERS * y + q, :, xs] = piece

    for part in range(side_bands):
        for hop in range(1, devices):
            copy_a(part, hop).wait_send()
        for side in range(2):
            for step in range(groups):
                pl.when(me != 2 * step + side)(copy_e(side, part, step).wait_send)

    @pl.when(crossed)
    def _():
        for part in range(side_bands):
            for core in range(2):
                detour(core, part).wait_send()
                direct(core, part).wait_send()

    @pl.when(jnp.logical_not(crossed))
    def _():
        half.wait_send()
        for part in range(side_bands):
            for core in range(2):
                onward(core, part).wait_send()

    for turn in range(4):
        for band in range(bands):
            halo(turn, band, 1).wait_send()
            pl.when(outer)(halo(turn, band, 0).wait_send)


def slab_shards(view_a, view_b_own, spread_a, spread_b):
    groups = lax.axis_size("gz")
    deep, tall, long_x = view_a.shape
    devices = 2 * groups
    wide = long_x // devices
    full_y, full_z = 2 * tall, view_b_own.shape[2]
    taps = spread_a.shape[1]
    radius = (taps - 1) // 2
    f32, bf16 = jnp.float32, jnp.bfloat16
    volume = pltpu.VMEM((wide, full_y, full_z), f32)
    rows_y = tall // QUARTERS
    bands, halves = full_y // BAND, tall // BAND
    dma = pltpu.SemaphoreType.DMA
    turned = pl.pallas_call(
        deconvolve,
        out_shape=jax.ShapeDtypeStruct((tall, deep, long_x), f32),
        in_specs=[pl.BlockSpec(memory_space=pl.ANY)] * 4,
        out_specs=pl.BlockSpec(memory_space=pltpu.VMEM),
        scratch_shapes=[
            pltpu.VMEM(view_a.shape, f32), pltpu.VMEM(view_b_own.shape, f32),
            pltpu.SMEM(spread_a.shape, f32), pltpu.SMEM(spread_b.shape, f32),
            pltpu.VMEM((devices, rows_y, deep, LANES), f32),
            pltpu.VMEM((2, rows_y, full_z, LANES), f32),
            pltpu.VMEM((2, wide, tall, full_z), f32),
            pltpu.VMEM((2, halves, wide // 2, BAND, full_z), f32),
            volume, volume, volume, volume,
            pltpu.VMEM((4, wide + 2 * radius, full_y, full_z), f32),
            pltpu.VMEM((2, rows_y, full_z, LANES), f32),
            pltpu.VMEM((devices, rows_y, deep, LANES), f32),
            pltpu.VMEM((4, 2 * full_z, 2 * full_z), bf16), pltpu.VMEM((4, 2 * LANES, 2 * LANES), bf16),
            dma((4,)), dma((halves, devices)), dma((halves, devices)), dma((2, 2, halves)), dma((2, 2, halves)), dma((2, halves)), dma((2, halves)),
            dma((4, bands, 2)), dma((4, bands, 2)), dma((halves, devices)), dma((halves, devices)),
        ],
        compiler_params=pltpu.CompilerParams(
            collective_id=0, has_side_effects=True, vmem_limit_bytes=48 * 1024 * 1024
        ),
    )(*(pltpu.with_memory_space_constraint(x, pltpu.HBM) for x in (view_a, view_b_own, spread_a, spread_b)))
    return jnp.transpose(turned, (1, 0, 2))


def fits_slabs(mesh, view_a, view_b_own, spread_a):
    groups, sides = mesh.shape["gz"], mesh.shape["gy"]
    deep = view_a[0] // (mesh.shape["blocks"] * groups)
    tall, wide = view_a[1] // sides, view_a[2] // (2 * groups)
    return (
        mesh.shape["blocks"] == 2 and groups % 2 == 0 and sides == 2 and wide * QUARTERS == LANES and view_b_own[2] == LANES and 4 * view_a[1] == LANES
        and tall % (8 * sides) == 0 and deep % 8 == 0 and spread_a[1] % 2 == 1 and spread_a[1] // 2 <= wide // 2
    )


def solution(mesh):
    in_specs = (P(("blocks", "gz"), "gy", None), P(("blocks", "gz"), "gy", None), P(), P())
    out_specs = P(("blocks", "gz"), "gy", None)

    def run(view_a, view_b_own, spread_a, spread_b):
        plan = slab_shards if fits_slabs(mesh, view_a.shape, view_b_own.shape, spread_a.shape) else shards
        split_plan = jax.shard_map(plan, mesh=mesh, in_specs=in_specs, out_specs=out_specs, check_vma=False)
        return split_plan(view_a, view_b_own, spread_a, spread_b)

    return run
```
